32 devices in a mesh: tm: 4 (over y, x), sky: 8 (over z, core).
Axes of the slice: x: 2, y: 2, z: 4, core: 2. Of those that a mesh axis runs over, the one named last changes fastest.
Arguments:
- residual: float32 [16384, 128], P(('tm', 'sky')), may hold values from -110 to 110
- obs_weight: float32 [16384, 128], P(('tm', 'sky')), may hold values from 0.5 to 2
- source_partials: float32 [5, 16384, 128], P(None, ('tm', 'sky')), may hold values from -1 to 1
- attitude_partials: float32 [16, 16384, 128], P(None, ('tm', 'sky')), may hold values from -1.5 to 1.5
- source_index: int32 [16384, 128], P(('tm', 'sky')), may hold values from 0 to 127
- tile_pixel: int32 [16384], P(('tm', 'sky')), may hold values from 0 to 1023, as said below
- tile_knot: int32 [16384], P(('tm', 'sky')), may hold values from 0 to 2047, as said below
- pixel_slot: int32 [1024], replicated, may hold values from 0 to 1023, as said below
Outputs:
- final_residual: float32 [16384, 128], P(('tm', 'sky'))
- source_update: float32 [5, 131072], P(None, 'sky')
- attitude_update: float32 [4, 2048], P(None, 'tm')
The draws below stay inside these ranges and needn't reach their ends.
Inputs may be any that keep to these rules, and one draw needn't show every extreme that they name: Tiles come in aligned blocks of 512; with owner = pixel_slot[tile_pixel[t]] // 128, no block holds more than 192 tiles of one owner, and every block holds exactly 192 tiles of some owner. `pixel_slot`: every slot number appears once. `tile_knot`: the tiles of aligned block q of 512 tiles have first knots in [q * 64, (q + 1) * 64).
All inputs are finite; a program needn't handle non-finite values.
Results may differ from the reference program's by a relative error of at most 0.0003.
Values sent between devices are 32-bit elements; how exact they have to be, the bound alone decides.
A program may use at most 128 MiB of HBM per device.

```python
import math
import jax
import jax.numpy as jnp
from jax import lax

OBS_TILE = 128
TILES_DEV = 512
PIX_DEV = 128
SRC_PIX = 128
OWNERS = 8
TIME_SHARDS = 4
CAP = 192
SPAN = 64
PIXELS = 1024
KNOTS = 2048
TILES = 16384


def sky_layout(key):
    slot_of_pixel = jax.random.permutation(jax.random.fold_in(key, 11), PIXELS).astype(jnp.int32)
    pixel_of_slot = jnp.argsort(slot_of_pixel, stable=True).astype(jnp.int32)
    blocks = TILES // TILES_DEV
    crowded_rows = jax.random.randint(jax.random.fold_in(key, 12), (TIME_SHARDS,), 0, OWNERS)
    crowded = crowded_rows[jnp.arange(blocks, dtype=jnp.int32) // OWNERS]
    positions = jnp.arange(TILES_DEV, dtype=jnp.int32)
    remaining = positions - CAP
    plain_owner = (crowded[:, None] + 1 + remaining[None, :] % (OWNERS - 1)) % OWNERS
    owner_ids = jnp.where(positions[None, :] < CAP, crowded[:, None], plain_owner)
    shuffles = jax.vmap(lambda sub: jax.random.permutation(sub, TILES_DEV))(jax.random.split(jax.random.fold_in(key, 13), blocks))
    owner_ids = jnp.take_along_axis(owner_ids, shuffles, axis=1)
    local_pixel = jax.random.randint(jax.random.fold_in(key, 14), (blocks, TILES_DEV), 0, PIX_DEV)
    pixel_ids = pixel_of_slot[(owner_ids * PIX_DEV + local_pixel).reshape(-1)]
    return (slot_of_pixel, pixel_ids.astype(jnp.int32))


def draw_pixel_slot(key, part):
    return sky_layout(key)[0]


def draw_tile_pixel(key, part):
    return sky_layout(key)[1]


def knot_starts(key):
    offset = jax.random.randint(jax.random.fold_in(key, 21), (TILES,), 0, SPAN)
    return (jnp.arange(TILES, dtype=jnp.int32) // TILES_DEV * SPAN + offset).astype(jnp.int32)


def draw_tile_knot(key, part):
    return knot_starts(key)


def attitude_parts(key):
    partials = jnp.clip(0.25 * jax.random.normal(jax.random.fold_in(key, 31), (16, TILES, OBS_TILE), jnp.float32), -1.5, 1.5)
    return partials


def draw_attitude_partials(key, part):
    return attitude_parts(key)


def draw_residual(key, part):
    partials = attitude_parts(key)
    knot_start = knot_starts(key)
    attitude_curve = jnp.clip(jax.random.normal(jax.random.fold_in(key, 32), (4, KNOTS + 3), jnp.float32), -4.0, 4.0)
    signal = jnp.clip(jax.random.normal(jax.random.fold_in(key, 33), (TILES, OBS_TILE), jnp.float32), -6.0, 6.0)
    for segment in range(4):
        values = jnp.take(attitude_curve, knot_start + segment, axis=1)
        for component in range(4):
            signal = signal + partials[4 * segment + component] * values[component][:, None]
    return signal


def with_ends(values, rng, low, high):
    shape = values.shape
    spot = [jax.random.randint(jax.random.fold_in(rng, axis), (), 0, shape[axis]) for axis in range(len(shape))]
    values = values.at[tuple(spot)].set(low)
    longest = shape.index(max(shape))
    spot[longest] = (spot[longest] + 1) % shape[longest]
    return values.at[tuple(spot)].set(high)


def shard_levels(key, extent, cuts, low, top_value):
    gain, own = 1.0, jax.random.fold_in(key, 6)
    for axis_at, blocks in cuts:
        heights = jnp.exp(jax.random.uniform(jax.random.fold_in(own, axis_at), (blocks,), jnp.float32, low / len(cuts), top_value / len(cuts)))
        gain = gain * jnp.repeat(heights, extent[axis_at] // blocks).reshape([-1 if axis == axis_at else 1 for axis in range(len(extent))])
    return gain


def centred(own_key, extent, width, reach, cuts=(), kind=jnp.bfloat16):
    values = width * jax.random.normal(own_key, extent, jnp.float32)
    if cuts:
        values = values * shard_levels(own_key, extent, cuts, -0.22, 0.18)
    return jnp.clip(values, -reach, reach).astype(kind)


def setup_inputs(seed: int = 0) -> dict:
    arg_keys = jax.random.split(jax.random.key(seed), 9)
    return {
        "residual": draw_residual(jax.random.fold_in(arg_keys[8], 71), 0),
        "obs_weight": jnp.clip(jnp.exp(math.log(2.0) - 1.3862944 * jax.random.uniform(arg_keys[1], (TILES, OBS_TILE), jnp.float32) ** shard_levels(arg_keys[1], (TILES, OBS_TILE), ((0, 32),), -0.2, 0.2)), 0.5, 2.0),
        "source_partials": centred(arg_keys[2], (5, TILES, OBS_TILE), 32 ** -0.5, 1.0, ((1, 32),), jnp.float32),
        "attitude_partials": draw_attitude_partials(jax.random.fold_in(arg_keys[8], 71), 0),
        "source_index": with_ends(jax.random.randint(arg_keys[4], (TILES, OBS_TILE), 0, SRC_PIX), jax.random.fold_in(arg_keys[4], 1), 0, SRC_PIX - 1).astype(jnp.int32),
        "tile_pixel": draw_tile_pixel(jax.random.fold_in(arg_keys[8], 71), 0),
        "tile_knot": draw_tile_knot(jax.random.fold_in(arg_keys[8], 71), 0),
        "pixel_slot": draw_pixel_slot(jax.random.fold_in(arg_keys[8], 71), 0),
    }


SOURCE_PAIRS = tuple(((first, second) for first in range(5) for second in range(first, 5)))
KNOT_PAIRS = tuple(((first, second) for first in range(4) for second in range(first, 4)))

def damped_solve(normal, target, order, pairs):
    entries = {}
    for number, couple in enumerate(pairs):
        entries[couple] = normal[number]
    factor = {}
    for column in range(order):
        pivot_value = entries[column, column] + 1.0
        for earlier in range(column):
            pivot_value = pivot_value - factor[column, earlier] * factor[column, earlier]
        pivot_value = jnp.sqrt(pivot_value)
        factor[column, column] = pivot_value
        for below in range(column + 1, order):
            current = entries[column, below]
            for earlier in range(column):
                current = current - factor[below, earlier] * factor[column, earlier]
            factor[below, column] = current / pivot_value
    forward = []
    for column in range(order):
        current = target[column]
        for earlier in range(column):
            current = current - factor[column, earlier] * forward[earlier]
        forward.append(current / factor[column, column])
    answer = [None] * order
    for column in reversed(range(order)):
        current = forward[column]
        for later in range(column + 1, order):
            current = current - factor[later, column] * answer[later]
        answer[column] = current / factor[column, column]
    return jnp.stack(answer)

def source_terms(weights, partials, baseline):
    products = [weights * partials[first] * partials[second] for first, second in SOURCE_PAIRS]
    products = products + [weights * partials[first] * baseline for first in range(5)]
    return products

def knot_terms(weights, partials, baseline):
    result = []
    for segment in range(4):
        portion = partials[4 * segment:4 * segment + 4]
        sums_rows = [lax.optimization_barrier(jnp.sum(weights * portion[first] * portion[second], axis=-1)) for first, second in KNOT_PAIRS]
        sums_rows = sums_rows + [lax.optimization_barrier(jnp.sum(weights * portion[first] * baseline, axis=-1)) for first in range(4)]
        result.append(jnp.stack(sums_rows))
    return result

def correct(baseline, partials, picked):
    accumulated = partials[0] * picked[0]
    for component in range(1, partials.shape[0]):
        accumulated = accumulated + partials[component] * picked[component]
    return baseline - accumulated

def knot_correct(baseline, partials, extended, knot_start):
    accumulated = None
    for segment in range(4):
        values = jnp.take(extended, knot_start + segment, axis=1)
        for component in range(4):
            addend = partials[4 * segment + component] * values[component][:, None]
            accumulated = addend if accumulated is None else accumulated + addend
    return baseline - accumulated

def reference(residual, obs_weight, source_partials, attitude_partials, source_index, tile_pixel, tile_knot, pixel_slot):
    blocks = residual.shape[0] // TILES_DEV
    sources = pixel_slot.shape[0] * SRC_PIX
    source_id = (jnp.take(pixel_slot, tile_pixel)[:, None] * SRC_PIX + source_index).astype(jnp.int32)

    def add_block(running, number):
        offset = (number * TILES_DEV).astype(jnp.int32)
        baseline = lax.dynamic_slice_in_dim(residual, offset, TILES_DEV, 0)
        weights = lax.dynamic_slice_in_dim(obs_weight, offset, TILES_DEV, 0)
        partials = lax.dynamic_slice_in_dim(source_partials, offset, TILES_DEV, 1)
        indices = lax.dynamic_slice_in_dim(source_id, offset, TILES_DEV, 0)
        stacked = jnp.stack(source_terms(weights, partials, baseline), axis=-1).reshape(-1, 20)
        return (running + jax.ops.segment_sum(stacked, indices.reshape(-1), num_segments=sources), None)
    normals, _ = lax.scan(add_block, jnp.zeros((sources, 20), jnp.float32), jnp.arange(blocks, dtype=jnp.int32))
    normals = normals.T
    source_update = damped_solve(normals[:15], normals[15:], 5, SOURCE_PAIRS)
    picked = jnp.take(source_update, source_id, axis=1)
    settled = correct(residual, source_partials, picked)
    knots = KNOTS
    accumulated = jnp.zeros((14, knots + 3), jnp.float32)
    for segment, tile_sums in enumerate(knot_terms(obs_weight, attitude_partials, settled)):
        accumulated = accumulated + jax.ops.segment_sum(tile_sums.T, tile_knot + segment, num_segments=knots + 3).T
    attitude_update = damped_solve(accumulated[:10, :knots], accumulated[10:, :knots], 4, KNOT_PAIRS)
    extended = jnp.concatenate([attitude_update, jnp.zeros((4, 3), jnp.float32)], axis=1)
    final_residual = knot_correct(settled, attitude_partials, extended, tile_knot)
    return (final_residual, source_update, attitude_update)
```

```python
import functools

import jax
import jax.numpy as jnp
from jax import lax
from jax.experimental import pallas as pl
from jax.experimental.pallas import tpu as pltpu
from jax.sharding import PartitionSpec as P

KNOTS_DEV = 512
ROWS = 20
PAD = 24
UPD = 5
LANES = 128
SUB = 8
MIB = 1024 * 1024

SOURCE_PAIRS = tuple(((first, second) for first in range(5) for second in range(first, 5)))
KNOT_PAIRS = tuple(((first, second) for first in range(4) for second in range(first, 4)))


def damped_solve(normal, target, order, pairs):
    entries = {}
    for number, couple in enumerate(pairs):
        entries[couple] = normal[number]
    factor = {}
    for column in range(order):
        pivot_value = entries[column, column] + 1.0
        for earlier in range(column):
            pivot_value = pivot_value - factor[column, earlier] * factor[column, earlier]
        pivot_value = jnp.sqrt(pivot_value)
        factor[column, column] = pivot_value
        for below in range(column + 1, order):
            current = entries[column, below]
            for earlier in range(column):
                current = current - factor[below, earlier] * factor[column, earlier]
            factor[below, column] = current / pivot_value
    forward = []
    for column in range(order):
        current = target[column]
        for earlier in range(column):
            current = current - factor[column, earlier] * forward[earlier]
        forward.append(current / factor[column, column])
    answer = [None] * order
    for column in reversed(range(order)):
        current = forward[column]
        for later in range(column + 1, order):
            current = current - factor[later, column] * answer[later]
        answer[column] = current / factor[column, column]
    return answer


def split_times(times):
    inner = 2 if times % 2 == 0 else 1
    return times // inner, inner


def sums_kernel(times, owners, tiles_step, pixel_ref, slot_ref, resid, weight, parts, index, out, stage, prods):
    tiles = resid.shape[0]
    outer, inner = split_times(times)
    pixels = out.shape[0] // ROWS
    per_owner = pixels // owners
    run = per_owner // times
    half = run // 2
    zero = jnp.zeros((256, LANES), jnp.float32)

    def clear(step, carry):
        out[pl.ds(pl.multiple_of(step * 256, 256), 256), :] = zero
        return carry

    lax.fori_loop(0, pixels * ROWS // 256, clear, 0)
    stage[...] = jnp.zeros_like(stage)
    prods[...] = jnp.zeros_like(prods)
    sources = lax.broadcasted_iota(jnp.int32, (SUB, LANES), 0).astype(jnp.float32)
    bands = [
        jnp.concatenate([sources + float(16 * band), sources + float(16 * band + 8)], axis=0).astype(jnp.bfloat16)
        for band in range(LANES // 16)
    ]
    lanes_of = jnp.concatenate(bands, axis=0)
    one = jnp.ones((LANES, LANES), jnp.bfloat16)
    none = jnp.zeros((LANES, LANES), jnp.bfloat16)

    def place(tile):
        seat = slot_ref[pixel_ref[tile]]
        owner, rest = seat // per_owner, seat % per_owner
        time, spot = rest // run, rest % run
        low_half = spot // half
        time_out, time_in = time // inner, time % inner
        order = jnp.where(low_half == 0, time_in * outer + time_out, time)
        return (((owner * 2 + low_half) * times + order) * half + spot % half) * ROWS

    def accumulate(step, slot):
        for j in range(tiles_step):
            start = place(step * tiles_step + j)
            values = prods[pl.ds(slot * tiles_step * PAD + j * PAD, PAD), :]
            out[pl.ds(start, ROWS), :] += values[:ROWS]

    def multiply(step, slot):
        for part in range(tiles_step // SUB):
            base = pl.multiple_of(step * tiles_step + part * SUB, SUB)
            here = pl.ds(base, SUB)
            fields = [parts[c, here, :] for c in range(5)]
            scaled = [weight[here, :] * field for field in fields]
            baseline = resid[here, :]
            row = part * SUB * PAD
            for first, second in SOURCE_PAIRS:
                stage[pl.ds(row, SUB, stride=PAD), :] = scaled[first] * fields[second]
                row += 1
            for first in range(5):
                stage[pl.ds(row, SUB, stride=PAD), :] = scaled[first] * baseline
                row += 1
            ids = index[here, :].astype(jnp.float32)
            for j in range(SUB):
                number = part * SUB + j
                values = stage[number * PAD : (number + 1) * PAD, :]
                high = values.astype(jnp.bfloat16).astype(jnp.float32)
                both = jnp.concatenate([high, values - high], axis=0).astype(jnp.bfloat16)
                wide = jnp.broadcast_to(ids[j : j + 1, :], (16, LANES)).astype(jnp.bfloat16)
                hits = jnp.where(lanes_of == jnp.concatenate([wide] * (LANES // 16), axis=0), one, none)
                got = lax.dot_general(
                    both, hits, (((1,), (1,)), ((), ())), preferred_element_type=jnp.float32
                )
                prods[pl.ds(slot * tiles_step * PAD + number * PAD, PAD), :] = got[:PAD] + got[PAD:]

    steps = tiles // tiles_step
    multiply(0, 0)

    def pair(step, carry):
        multiply(2 * step + 1, 1)
        accumulate(2 * step, 0)
        multiply(jnp.minimum(2 * step + 2, steps - 1), 0)
        accumulate(2 * step + 1, 1)
        return carry

    lax.fori_loop(0, steps // 2, pair, 0)


def local_sums(tile_pixel, pixel_slot, residual, obs_weight, source_partials, source_index, times, owners):
    pixels = pixel_slot.shape[0]
    tiles_step = 16
    return pl.pallas_call(
        functools.partial(sums_kernel, times, owners, tiles_step),
        name="local_sums",
        out_shape=jax.ShapeDtypeStruct((pixels * ROWS, LANES), jnp.float32),
        in_specs=[pl.BlockSpec(memory_space=pltpu.SMEM)] * 2 + [pl.BlockSpec(memory_space=pltpu.VMEM)] * 4,
        out_specs=pl.BlockSpec(memory_space=pltpu.VMEM),
        scratch_shapes=[
            pltpu.VMEM((tiles_step * PAD, LANES), jnp.float32),
            pltpu.VMEM((2 * tiles_step * PAD, LANES), jnp.float32),
        ],
        compiler_params=pltpu.CompilerParams(vmem_limit_bytes=30 * MIB),
    )(tile_pixel, pixel_slot, residual, obs_weight, source_partials, source_index)


def add_rows(target, *sources):
    rows = target.shape[0]
    step_rows = 32
    while rows % step_rows:
        step_rows //= 2

    def one(step, carry):
        here = pl.ds(pl.multiple_of(step * step_rows, step_rows), step_rows)
        total = sources[0][here, :]
        for source in sources[1:]:
            total = total + source[here, :]
        target[here, :] = total
        return carry

    lax.fori_loop(0, rows // step_rows, one, 0)


def square_sums(weight, att, rows, first, last):
    lane = lax.broadcasted_iota(jnp.int32, (SUB, LANES), 1)

    def group(step, carry):
        here = pl.ds(pl.multiple_of(step * SUB, SUB), SUB)
        scale = weight[here, :]
        total = jnp.zeros((SUB, LANES), jnp.float32)
        for m in range(4):
            fields = [att[4 * m + c, here, :] for c in range(4)]
            scaled = [scale * field for field in fields]
            for number, (a, b) in enumerate(KNOT_PAIRS):
                value = jnp.sum(scaled[a] * fields[b], axis=1, keepdims=True)
                total = jnp.where(lane == 16 * m + number, value, total)
        rows[here, :] = total
        return carry

    lax.fori_loop(first, last, group, 0)


def exchange_kernel(
    times, lines, sums, weight, att, table, squares, got0, a1, b1, a2, b2, part, got2, upd, *sems
):
    s0, r0, sa1, ra1, sb1, rb1, sa2, ra2, sb2, rb2, s3, r3, su, ru, st, rt, sd, rd = sems
    outer, inner = split_times(times)
    mesh_ids = pl.DeviceIdType.MESH
    time, sky = lax.axis_index("tm"), lax.axis_index("sky")
    line, core = sky // 2, sky % 2
    mo, mi = time // inner, time % inner
    partner = (time, sky + 1 - 2 * core)
    half_rows = a2.shape[2]
    tiles = weight.shape[0]
    inner_at = [lax.rem(mi + step, inner) for step in range(1, inner)]
    outer_at = [lax.rem(mo + step, outer) for step in range(1, outer)]
    inner_peers = [(mo * inner + i, sky) for i in inner_at]
    outer_peers = [(o * inner + mi, sky) for o in outer_at]
    steps = sorted(range(1, lines), key=lambda step: -min(step, lines - step)) + [0]
    pieces = [lax.rem(line + step, lines) for step in steps]
    line_peers = [(time, piece * 2 + core) for piece in pieces[:-1]]

    barrier = pltpu.get_barrier_semaphore()
    peers = [partner] + inner_peers + outer_peers + line_peers
    for peer in peers:
        pl.semaphore_signal(barrier, inc=1, device_id=peer, device_id_type=mesh_ids)
    pl.semaphore_wait(barrier, len(peers))

    pending = []

    def send(source, target, send_sem, recv_sem, peer):
        copy = pltpu.make_async_remote_copy(
            src_ref=source, dst_ref=target, send_sem=send_sem, recv_sem=recv_sem,
            device_id=peer, device_id_type=mesh_ids,
        )
        copy.start()
        pending.append(copy)
        return copy

    count = len(pieces)
    zeroth = [
        send(sums.at[piece, 1 - core], got0.at[step], s0.at[step], r0.at[step], partner)
        for step, piece in enumerate(pieces)
    ]
    first_a, first_b, second_a, second_b, third = {}, {}, {}, {}, {}

    def stage_one(k):
        zeroth[k].wait_recv()
        for side in range(2):
            add_rows(got0.at[k, side], got0.at[k, side], sums.at[pieces[k], core, side])
            if side == 0:
                first_a[k] = [
                    send(
                        got0.at[k, 0, pl.ds(i * outer * half_rows, outer * half_rows)],
                        a1.at[k, number], sa1.at[k, number], ra1.at[k, number], peer,
                    )
                    for number, (i, peer) in enumerate(zip(inner_at, inner_peers))
                ]
            else:
                first_b[k] = [
                    send(
                        got0.at[k, 1, pl.ds(o * inner * half_rows, inner * half_rows)],
                        b1.at[k, number], sb1.at[k, number], rb1.at[k, number], peer,
                    )
                    for number, (o, peer) in enumerate(zip(outer_at, outer_peers))
                ]

    def stage_two(k):
        for copy in first_a[k]:
            copy.wait_recv()
        mine = got0.at[k, 0, pl.ds(mi * outer * half_rows, outer * half_rows)]
        if inner > 1:
            add_rows(mine, mine, *[a1.at[k, number] for number in range(inner - 1)])
        second_a[k] = [
            send(
                got0.at[k, 0, pl.ds((mi * outer + o) * half_rows, half_rows)],
                a2.at[k, number], sa2.at[k, number], ra2.at[k, number], peer,
            )
            for number, (o, peer) in enumerate(zip(outer_at, outer_peers))
        ]
        for copy in first_b[k]:
            copy.wait_recv()
        mine = got0.at[k, 1, pl.ds(mo * inner * half_rows, inner * half_rows)]
        if outer > 1:
            add_rows(mine, mine, *[b1.at[k, number] for number in range(outer - 1)])
        second_b[k] = [
            send(
                got0.at[k, 1, pl.ds((mo * inner + i) * half_rows, half_rows)],
                b2.at[k, number], sb2.at[k, number], rb2.at[k, number], peer,
            )
            for number, (i, peer) in enumerate(zip(inner_at, inner_peers))
        ]

    def stage_three(k):
        for copy in second_a[k]:
            copy.wait_recv()
        own = got0.at[k, 0, pl.ds((mi * outer + mo) * half_rows, half_rows)]
        add_rows(part.at[k, pl.ds(0, half_rows)], own, *[a2.at[k, number] for number in range(outer - 1)])
        for copy in second_b[k]:
            copy.wait_recv()
        own = got0.at[k, 1, pl.ds((mo * inner + mi) * half_rows, half_rows)]
        add_rows(
            part.at[k, pl.ds(half_rows, half_rows)], own, *[b2.at[k, number] for number in range(inner - 1)]
        )
        if k < count - 1:
            third[k] = send(part.at[k], got2.at[k], s3.at[k], r3.at[k], line_peers[k])

    groups = tiles // SUB
    stage_one(0)
    if count > 1:
        stage_one(1)
    square_sums(weight, att, squares, 0, groups // 2)
    for k in range(count):
        stage_two(k)
        if k + 2 < count:
            stage_one(k + 2)
        if k == 0:
            square_sums(weight, att, squares, groups // 2, groups)
        if k > 0:
            stage_three(k - 1)
    stage_three(count - 1)
    for k in range(count - 1):
        third[k].wait_recv()
    total = part.at[count - 1]
    add_rows(total, total, *[got2.at[k] for k in range(count - 1)])

    run = 2 * half_rows // ROWS
    block = run * UPD

    def solve(step, carry):
        base = step * SUB
        entry = [
            part[count - 1, pl.ds(base * ROWS + row, SUB, stride=ROWS), :] for row in range(ROWS)
        ]
        answer = damped_solve(entry[:15], entry[15:], 5, SOURCE_PAIRS)
        for c in range(UPD):
            upd[pl.ds(base * UPD + c, SUB, stride=UPD), :] = answer[c]
        return carry

    lax.fori_loop(0, run // SUB, solve, 0)

    half_block = block // 2

    def spot(source_line, source_core, source_time):
        return pl.multiple_of(((source_line * 2 + source_core) * times + source_time) * block, SUB)

    own = table.at[pl.ds(spot(line, core, time), block)]
    from_line = []
    for number, peer in enumerate(line_peers):
        from_line.append(send(upd, own, su.at[number], ru.at[number], peer))
    sources = [lax.rem(line + lines - step, lines) for step in steps[:-1]]
    order = [count - 1] + sorted(range(count - 1), key=lambda n: min(steps[n], lines - steps[n]))
    near, far = {}, {}

    def spread(n):
        source = line if n == count - 1 else sources[n]
        place = table.at[pl.ds(spot(source, core, time), block)]
        if n < count - 1:
            from_line[n].wait_recv()
            held = place
        else:
            held = upd
        near[n] = [
            send(held, place, st.at[n, number], rt.at[n, number], peer)
            for number, peer in enumerate(inner_peers + outer_peers)
        ]
        return source

    def relay(n, source):
        far[n] = []
        number = inner + outer - 2
        for which, copy in enumerate(near[n]):
            copy.wait_recv()
            from_inner = which < inner - 1
            if from_inner:
                origin = mo * inner + lax.rem(mi + inner - (which + 1), inner)
                rows, targets = 0, outer_peers
            else:
                origin = lax.rem(mo + outer - (which - inner + 2), outer) * inner + mi
                rows, targets = half_block, inner_peers
            piece = table.at[pl.ds(spot(source, core, origin) + rows, half_block)]
            for peer in targets:
                far[n].append(send(piece, piece, st.at[n, number], rt.at[n, number], peer))
                number += 1

    def finish(n, source):
        for copy in far[n]:
            copy.wait_recv()
        place = table.at[pl.ds(spot(source, core, 0), times * block)]
        return send(place, place, sd.at[n], rd.at[n], partner)

    held_rows = pl.multiple_of(spot(line, core, time), SUB)
    spread_sources = {order[0]: spread(order[0])}
    table[pl.ds(held_rows, block), :] = upd[...]
    last = []
    for at, n in enumerate(order):
        if at + 1 < count:
            spread_sources[order[at + 1]] = spread(order[at + 1])
        relay(n, spread_sources[n])
        if at > 0:
            last.append(finish(order[at - 1], spread_sources[order[at - 1]]))
    last.append(finish(order[-1], spread_sources[order[-1]]))
    for copy in last:
        copy.wait_recv()
    for copy in pending:
        copy.wait_send()


def exchange(sums, obs_weight, attitude_partials):
    times, owners = lax.axis_size("tm"), lax.axis_size("sky")
    lines = owners // 2
    outer, inner = split_times(times)
    total_rows = sums.shape[0]
    half_rows = total_rows // (owners * times * 2)
    pixels = total_rows // ROWS
    block = pixels // (owners * times) * UPD
    tiles = obs_weight.shape[0]
    dma = pltpu.SemaphoreType.DMA
    vmem = pltpu.VMEM
    near = inner + outer - 2
    far = 2 * (inner - 1) * (outer - 1)
    f32 = jnp.float32

    def pair(*shape):
        return [dma(shape), dma(shape)]

    return pl.pallas_call(
        functools.partial(exchange_kernel, times, lines),
        name="exchange",
        out_shape=(
            jax.ShapeDtypeStruct((pixels * UPD + SUB, LANES), f32),
            jax.ShapeDtypeStruct((tiles, LANES), f32),
        ),
        in_specs=[pl.BlockSpec(memory_space=pltpu.VMEM)] * 3,
        out_specs=(pl.BlockSpec(memory_space=pltpu.VMEM),) * 2,
        scratch_shapes=[
            vmem((lines, 2, times * half_rows, LANES), f32),
            vmem((lines, max(inner - 1, 1), outer * half_rows, LANES), f32),
            vmem((lines, max(outer - 1, 1), inner * half_rows, LANES), f32),
            vmem((lines, max(outer - 1, 1), half_rows, LANES), f32),
            vmem((lines, max(inner - 1, 1), half_rows, LANES), f32),
            vmem((lines, 2 * half_rows, LANES), f32),
            vmem((max(lines - 1, 1), 2 * half_rows, LANES), f32),
            vmem((block, LANES), f32),
        ]
        + pair(lines)
        + pair(lines, max(inner - 1, 1))
        + pair(lines, max(outer - 1, 1))
        + pair(lines, max(outer - 1, 1))
        + pair(lines, max(inner - 1, 1))
        + pair(lines)
        + pair(lines)
        + pair(lines, near + far)
        + pair(lines),
        compiler_params=pltpu.CompilerParams(
            collective_id=0, has_side_effects=True, vmem_limit_bytes=44 * MIB
        ),
    )(sums.reshape(lines, 2, 2, times * half_rows, LANES), obs_weight, attitude_partials)


def thirds(value):
    high = value.astype(jnp.bfloat16)
    rest = value - high.astype(jnp.float32)
    middle = rest.astype(jnp.bfloat16)
    return high, middle, (rest - middle.astype(jnp.float32)).astype(jnp.bfloat16)


def settle_kernel(pixel_ref, slot_ref, knots, resid, weight, parts, att, index, table, squares, out, sums, rows, terms):
    tiles = resid.shape[0]
    lane = lax.broadcasted_iota(jnp.int32, (SUB, LANES), 1)

    def group(step, carry):
        base = pl.multiple_of(step * SUB, SUB)
        here = pl.ds(base, SUB)
        for j in range(SUB):
            seat = slot_ref[pixel_ref[base + j]]
            rows[j * SUB : (j + 1) * SUB, :] = table[pl.ds(seat * UPD, SUB), :]
        ids = index[here, :]
        total = None
        for c in range(UPD):
            picked = jnp.take_along_axis(rows[pl.ds(c, SUB, stride=SUB), :], ids, axis=1)
            addend = parts[c, here, :] * picked
            total = addend if total is None else total + addend
        settled = resid[here, :] - total
        out[here, :] = settled
        scaled = weight[here, :] * settled
        term = squares[here, :]
        for m in range(4):
            for c in range(4):
                value = jnp.sum(scaled * att[4 * m + c, here, :], axis=1, keepdims=True)
                term = jnp.where(lane == 16 * m + 10 + c, value, term)
        terms[here, :] = term
        return carry

    lax.fori_loop(0, tiles // SUB, group, 0)
    knot = lax.broadcasted_iota(jnp.int32, (LANES, tiles), 0)
    hits = jnp.where(knot == knots[...], 1.0, 0.0).astype(jnp.bfloat16)
    placed = None
    for piece in thirds(terms[...]):
        got = jnp.dot(hits, piece, preferred_element_type=jnp.float32)
        placed = got if placed is None else placed + got
    turned = placed.T
    total = turned[:16]
    for m in range(1, 4):
        total = total + pltpu.roll(turned[16 * m : 16 * m + 16], m, 1)
    sums[...] = total


def settle(tile_pixel, pixel_slot, knots, residual, obs_weight, source_partials, attitude_partials, source_index, table, squares):
    tiles = residual.shape[0]
    return pl.pallas_call(
        settle_kernel,
        name="settle",
        out_shape=(
            jax.ShapeDtypeStruct(residual.shape, jnp.float32),
            jax.ShapeDtypeStruct((16, LANES), jnp.float32),
        ),
        in_specs=[pl.BlockSpec(memory_space=pltpu.SMEM)] * 2 + [pl.BlockSpec(memory_space=pltpu.VMEM)] * 8,
        out_specs=(pl.BlockSpec(memory_space=pltpu.VMEM),) * 2,
        scratch_shapes=[pltpu.VMEM((SUB * SUB, LANES), jnp.float32), pltpu.VMEM((tiles, LANES), jnp.float32)],
        compiler_params=pltpu.CompilerParams(vmem_limit_bytes=32 * MIB),
    )(tile_pixel, pixel_slot, knots, residual, obs_weight, source_partials, attitude_partials, source_index, table, squares)


def finish_kernel(
    times, owners, span, sums, knots, settled, att, table, out, source_out, knot_out,
    before, mine, others, after, values, sa, ra, sb, rb, sc, rc,
):
    mesh_ids = pl.DeviceIdType.MESH
    time, sky = lax.axis_index("tm"), lax.axis_index("sky")
    blocks = times * owners
    block = time * owners + sky
    nxt, prev = lax.rem(block + 1, blocks), lax.rem(block + blocks - 1, blocks)
    next_id, prev_id = (nxt // owners, lax.rem(nxt, owners)), (prev // owners, lax.rem(prev, owners))
    peers = [(time, lax.rem(sky + step, owners)) for step in range(1, owners)]

    barrier = pltpu.get_barrier_semaphore()
    for peer in [next_id, prev_id] + peers:
        pl.semaphore_signal(barrier, inc=1, device_id=peer, device_id_type=mesh_ids)
    pl.semaphore_wait(barrier, owners + 1)

    pending = []

    def send(source, target, send_sem, recv_sem, peer):
        copy = pltpu.make_async_remote_copy(
            src_ref=source, dst_ref=target, send_sem=send_sem, recv_sem=recv_sem,
            device_id=peer, device_id_type=mesh_ids,
        )
        copy.start()
        pending.append(copy)
        return copy

    handed = send(sums, before, sa, ra, next_id)

    per_owner = source_out.shape[1] // LANES

    def spread(pixel, carry):
        place = pl.ds(pl.multiple_of(pixel * LANES, LANES), LANES)
        source_out[:, place] = table[pl.ds((sky * per_owner + pixel) * UPD, UPD), :]
        return carry

    lax.fori_loop(0, per_owner, spread, 0)

    lane = lax.broadcasted_iota(jnp.int32, (16, LANES), 1)
    handed.wait_recv()
    arrived = pltpu.roll(before[...], LANES - span, 1)
    arrived = jnp.where((lane < 3) & (block > 0), arrived, 0.0)
    whole = jnp.where(lane < span, sums[...], 0.0) + arrived
    answer = damped_solve(
        [whole[n : n + 1] for n in range(10)], [whole[n : n + 1] for n in range(10, 14)], 4, KNOT_PAIRS
    )
    for c in range(4):
        mine[c : c + 1, :] = answer[c]
        mine[4 + c : 5 + c, :] = answer[c]
    back = send(mine, after, sb, rb, prev_id)
    around = [
        send(mine, others.at[sky], sc.at[number], rc.at[number], peer)
        for number, peer in enumerate(peers)
    ]
    back.wait_recv()
    lane = lax.broadcasted_iota(jnp.int32, (SUB, LANES), 1)
    following = jnp.where(block < blocks - 1, after[...], 0.0)
    extended = jnp.where(lane < span, mine[...], 0.0)
    extended = extended + jnp.where(
        (lane >= span) & (lane < span + 3), pltpu.roll(following, span, 1), 0.0
    )
    windows = []
    for m in range(0, 4, 2):
        low = extended if m == 0 else pltpu.roll(extended, LANES - m, 1)
        high = pltpu.roll(extended, LANES - m - 1, 1)
        half = lax.broadcasted_iota(jnp.int32, (SUB, LANES), 0) < 4
        windows.append(jnp.where(half, low, high))
    window = jnp.concatenate(windows, axis=0)
    tiles = settled.shape[0]
    knot = lax.broadcasted_iota(jnp.int32, (LANES, tiles), 0)
    hits = jnp.where(knot == knots[...], 1.0, 0.0).astype(jnp.bfloat16)
    picked = None
    for piece in thirds(window):
        got = jnp.dot(piece, hits, preferred_element_type=jnp.float32)
        picked = got if picked is None else picked + got
    for part in range(tiles // LANES):
        values[part * LANES : (part + 1) * LANES, :] = picked[:, part * LANES : (part + 1) * LANES].T

    def group(step, carry):
        here = pl.ds(pl.multiple_of(step * SUB, SUB), SUB)
        column = values[here, :]
        total = None
        for number in range(16):
            addend = att[number, here, :] * column[:, number : number + 1]
            total = addend if total is None else total + addend
        out[here, :] = settled[here, :] - total
        return carry

    lax.fori_loop(0, tiles // SUB, group, 0)
    for copy in around:
        copy.wait_recv()
    others[pl.ds(sky, 1)] = mine[...][None]
    each = LANES // span
    for first in range(0, owners, each):
        joined = jnp.where(lane < span, others[first], 0.0)
        for number in range(1, each):
            moved = pltpu.roll(others[first + number], number * span, 1)
            keep = (lane >= number * span) & (lane < (number + 1) * span)
            joined = jnp.where(keep, moved, joined)
        knot_out[:, first * span : first * span + LANES] = joined[:4]
    for copy in pending:
        copy.wait_send()


def finish(sums, knots, settled, attitude_partials, table, span):
    times, owners = lax.axis_size("tm"), lax.axis_size("sky")
    tiles = settled.shape[0]
    dma = pltpu.SemaphoreType.DMA
    f32 = jnp.float32
    pixels = (table.shape[0] - SUB) // UPD
    return pl.pallas_call(
        functools.partial(finish_kernel, times, owners, span),
        name="finish",
        out_shape=(
            jax.ShapeDtypeStruct(settled.shape, f32),
            jax.ShapeDtypeStruct((UPD, pixels // owners * LANES), f32),
            jax.ShapeDtypeStruct((4, span * owners), f32),
        ),
        in_specs=[pl.BlockSpec(memory_space=pltpu.VMEM)] * 5,
        out_specs=(pl.BlockSpec(memory_space=pltpu.VMEM),) * 3,
        scratch_shapes=[
            pltpu.VMEM((16, LANES), f32),
            pltpu.VMEM((SUB, LANES), f32),
            pltpu.VMEM((owners, SUB, LANES), f32),
            pltpu.VMEM((SUB, LANES), f32),
            pltpu.VMEM((tiles, 16), f32),
            dma, dma, dma, dma, dma((owners - 1,)), dma((owners - 1,)),
        ],
        compiler_params=pltpu.CompilerParams(
            collective_id=1, has_side_effects=True, vmem_limit_bytes=32 * MIB
        ),
    )(sums, knots, settled, attitude_partials, table)


def body(residual, obs_weight, source_partials, attitude_partials, source_index, tile_pixel, tile_knot, pixel_slot):
    owners = lax.axis_size("sky")
    times = lax.axis_size("tm")
    span = KNOTS_DEV // owners
    block = lax.axis_index("tm") * owners + lax.axis_index("sky")
    knots = (tile_knot - block * span)[None, :]
    sums = local_sums(
        tile_pixel, pixel_slot, residual, obs_weight, source_partials, source_index, times, owners
    )
    table, squares = exchange(sums, obs_weight, attitude_partials)
    settled, knot_sums = settle(
        tile_pixel, pixel_slot, knots, residual, obs_weight, source_partials, attitude_partials,
        source_index, table, squares,
    )
    return finish(knot_sums, knots, settled, attitude_partials, table, span)


def solution(mesh):
    in_specs = (
        P(("tm", "sky"), None),
        P(("tm", "sky"), None),
        P(None, ("tm", "sky"), None),
        P(None, ("tm", "sky"), None),
        P(("tm", "sky"), None),
        P(("tm", "sky")),
        P(("tm", "sky")),
        P(),
    )
    out_specs = (P(("tm", "sky"), None), P(None, "sky"), P(None, "tm"))
    return jax.shard_map(body, mesh=mesh, in_specs=in_specs, out_specs=out_specs, check_vma=False)
```

```python
import functools

import jax
import jax.numpy as jnp
from jax import lax
from jax.experimental import pallas as pl
from jax.experimental.pallas import tpu as pltpu
from jax.sharding import PartitionSpec as P

KNOTS_DEV = 512
ROWS = 20
PAD = 24
UPD = 5
LANES = 128
SUB = 8
MIB = 1024 * 1024

SOURCE_PAIRS = tuple(((first, second) for first in range(5) for second in range(first, 5)))
KNOT_PAIRS = tuple(((first, second) for first in range(4) for second in range(first, 4)))


def damped_solve(normal, target, order, pairs):
    entries = {}
    for number, couple in enumerate(pairs):
        entries[couple] = normal[number]
    factor = {}
    for column in range(order):
        pivot_value = entries[column, column] + 1.0
        for earlier in range(column):
            pivot_value = pivot_value - factor[column, earlier] * factor[column, earlier]
        pivot_value = jnp.sqrt(pivot_value)
        factor[column, column] = pivot_value
        for below in range(column + 1, order):
            current = entries[column, below]
            for earlier in range(column):
                current = current - factor[below, earlier] * factor[column, earlier]
            factor[below, column] = current / pivot_value
    forward = []
    for column in range(order):
        current = target[column]
        for earlier in range(column):
            current = current - factor[column, earlier] * forward[earlier]
        forward.append(current / factor[column, column])
    answer = [None] * order
    for column in reversed(range(order)):
        current = forward[column]
        for later in range(column + 1, order):
            current = current - factor[later, column] * answer[later]
        answer[column] = current / factor[column, column]
    return answer


def split_times(times):
    inner = 2 if times % 2 == 0 else 1
    return times // inner, inner


def sums_kernel(
    tiles_step, pixel_hbm, slot_hbm, resid_hbm, weight_hbm, parts_hbm, index_hbm, out,
    pixel_ref, slot_ref, resid, weight, parts, index, stage, prods, sems,
):
    copies = [
        pltpu.make_async_copy(source, target, sems.at[number])
        for number, (source, target) in enumerate(
            [
                (pixel_hbm, pixel_ref),
                (slot_hbm, slot_ref),
                (resid_hbm, resid),
                (weight_hbm, weight),
                (parts_hbm, parts),
                (index_hbm, index),
            ]
        )
    ]
    for copy in copies:
        copy.start()
    tiles = resid.shape[0]
    zero = jnp.zeros((256, LANES), jnp.float32)

    def clear(step, carry):
        out[pl.ds(pl.multiple_of(step * 256, 256), 256), :] = zero
        return carry

    lax.fori_loop(0, out.shape[0] // 256, clear, 0)
    stage[...] = jnp.zeros_like(stage)
    sources = lax.broadcasted_iota(jnp.int32, (SUB, LANES), 0).astype(jnp.float32)
    bands = [
        jnp.concatenate([sources + float(16 * band), sources + float(16 * band + 8)], axis=0).astype(jnp.bfloat16)
        for band in range(LANES // 16)
    ]
    lanes_of = jnp.concatenate(bands, axis=0)
    one = jnp.ones((LANES, LANES), jnp.bfloat16)
    none = jnp.zeros((LANES, LANES), jnp.bfloat16)
    blank = jnp.zeros((2 * PAD, LANES), jnp.bfloat16)
    for copy in copies:
        copy.wait()

    def accumulate(step, slot):
        for j in range(tiles_step):
            start = slot_ref[pixel_ref[step * tiles_step + j]] * ROWS
            values = prods[pl.ds(slot * tiles_step * PAD + j * PAD, PAD), :]
            out[pl.ds(start, ROWS), :] += values[:ROWS]

    def multiply(step, slot):
        for part in range(tiles_step // SUB):
            base = pl.multiple_of(step * tiles_step + part * SUB, SUB)
            here = pl.ds(base, SUB)
            fields = [parts[c, here, :] for c in range(5)]
            scaled = [weight[here, :] * field for field in fields]
            baseline = resid[here, :]
            row = part * SUB * PAD
            for first, second in SOURCE_PAIRS:
                stage[pl.ds(row, SUB, stride=PAD), :] = scaled[first] * fields[second]
                row += 1
            for first in range(5):
                stage[pl.ds(row, SUB, stride=PAD), :] = scaled[first] * baseline
                row += 1
            ids = index[here, :].astype(jnp.float32)
            for j in range(0, SUB, 2):
                row = (part * SUB + j) * PAD
                lhs, hits = [], []
                for side in range(2):
                    values = stage[row + side * PAD : row + (side + 1) * PAD, :]
                    high = values.astype(jnp.bfloat16).astype(jnp.float32)
                    both = jnp.concatenate([high, values - high], axis=0).astype(jnp.bfloat16)
                    lhs.append(jnp.concatenate([both, blank] if side == 0 else [blank, both], axis=1))
                    wide = jnp.broadcast_to(ids[j + side : j + side + 1, :], (16, LANES)).astype(jnp.bfloat16)
                    tall = jnp.concatenate([wide] * (LANES // 16), axis=0)
                    hits.append(jnp.where(lanes_of == tall, one, none))
                got = lax.dot_general(
                    jnp.concatenate(lhs, axis=0),
                    jnp.concatenate(hits, axis=1),
                    (((1,), (1,)), ((), ())),
                    preferred_element_type=jnp.float32,
                )
                for side in range(2):
                    low = 2 * side * PAD
                    prods[pl.ds(slot * tiles_step * PAD + row + side * PAD, PAD), :] = (
                        got[low : low + PAD] + got[low + PAD : low + 2 * PAD]
                    )

    steps = tiles // tiles_step
    multiply(0, 0)

    def pair(step, carry):
        multiply(2 * step + 1, 1)
        accumulate(2 * step, 0)
        multiply(jnp.minimum(2 * step + 2, steps - 1), 0)
        accumulate(2 * step + 1, 1)
        return carry

    lax.fori_loop(0, steps // 2, pair, 0)


def local_sums(tile_pixel, pixel_slot, residual, obs_weight, source_partials, source_index):
    pixels = pixel_slot.shape[0]
    tiles_step = 16
    return pl.pallas_call(
        functools.partial(sums_kernel, tiles_step),
        name="local_sums",
        out_shape=jax.ShapeDtypeStruct((pixels * ROWS, LANES), jnp.float32),
        in_specs=[pl.BlockSpec(memory_space=pltpu.HBM)] * 6,
        out_specs=pl.BlockSpec(memory_space=pltpu.VMEM),
        scratch_shapes=[
            pltpu.SMEM(tile_pixel.shape, jnp.int32),
            pltpu.SMEM(pixel_slot.shape, jnp.int32),
            pltpu.VMEM(residual.shape, jnp.float32),
            pltpu.VMEM(obs_weight.shape, jnp.float32),
            pltpu.VMEM(source_partials.shape, jnp.float32),
            pltpu.VMEM(source_index.shape, jnp.int32),
            pltpu.VMEM((tiles_step * PAD, LANES), jnp.float32),
            pltpu.VMEM((2 * tiles_step * PAD, LANES), jnp.float32),
            pltpu.SemaphoreType.DMA((6,)),
        ],
        compiler_params=pltpu.CompilerParams(vmem_limit_bytes=18 * MIB),
    )(*[pltpu.with_memory_space_constraint(v, pltpu.HBM) for v in (tile_pixel, pixel_slot, residual, obs_weight, source_partials, source_index)])


def add_rows(target, *sources):
    rows = target.shape[0]
    step_rows = next(size for size in range(160, 0, -SUB) if rows % size == 0)

    def one(step, carry):
        here = pl.ds(pl.multiple_of(step * step_rows, step_rows), step_rows)
        total = sources[0][here, :]
        for source in sources[1:]:
            total = total + source[here, :]
        target[here, :] = total
        return carry

    lax.fori_loop(0, rows // step_rows, one, 0)


def square_sums(weight, att, rows, first, last):
    lane = lax.broadcasted_iota(jnp.int32, (SUB, LANES), 1)

    def group(step, carry):
        for part in range(2):
            here = pl.ds(pl.multiple_of(step * 2 * SUB + part * SUB, SUB), SUB)
            scale = weight[here, :]
            total = jnp.zeros((SUB, LANES), jnp.float32)
            for m in range(4):
                fields = [att[4 * m + c, here, :] for c in range(4)]
                scaled = [scale * field for field in fields]
                for number, (a, b) in enumerate(KNOT_PAIRS):
                    value = jnp.sum(scaled[a] * fields[b], axis=1, keepdims=True)
                    total = jnp.where(lane == 16 * m + number, value, total)
            rows[here, :] = total
        return carry

    lax.fori_loop(first, last, group, 0)


def exchange_kernel(
    times, lines, subs, depth, sums, weight, att, table, squares, got0, a1, b1, a2, b2, part, got2, upd, *sems
):
    s0, r0, sa1, ra1, sb1, rb1, sa2, ra2, sb2, rb2, s3, r3, su, ru, st, rt, sd, rd = sems
    outer, inner = split_times(times)
    mesh_ids = pl.DeviceIdType.MESH
    time, sky = lax.axis_index("tm"), lax.axis_index("sky")
    line, core = sky // 2, sky % 2
    mo, mi = time // inner, time % inner
    partner = (time, sky + 1 - 2 * core)
    quarter = a2.shape[2]
    tiles = weight.shape[0]
    inner_at = [lax.rem(mi + step, inner) for step in range(1, inner)]
    outer_at = [lax.rem(mo + step, outer) for step in range(1, outer)]
    inner_peers = [(mo * inner + i, sky) for i in inner_at]
    outer_peers = [(o * inner + mi, sky) for o in outer_at]
    masks = list(range(lines - 1, 0, -1))
    line_of = {mask: jnp.bitwise_xor(line, mask) for mask in range(lines)}
    line_peer = {mask: (time, line_of[mask] * 2 + core) for mask in masks}

    barrier = pltpu.get_barrier_semaphore()
    peers = [partner] + inner_peers + outer_peers + [line_peer[mask] for mask in masks]
    for peer in peers:
        pl.semaphore_signal(barrier, inc=1, device_id=peer, device_id_type=mesh_ids)
    pl.semaphore_wait(barrier, len(peers))

    pending = []

    def send(source, target, send_sem, recv_sem, peer):
        copy = pltpu.make_async_remote_copy(
            src_ref=source, dst_ref=target, send_sem=send_sem, recv_sem=recv_sem,
            device_id=peer, device_id_type=mesh_ids,
        )
        copy.start()
        pending.append(copy)
        return copy

    pieces = [(mask, sub) for mask in masks + [0] for sub in range(subs)]
    count = len(pieces)
    zeroth = [
        send(sums.at[line_of[mask], 1 - core, :, sub], got0.at[k], s0.at[k], r0.at[k], partner)
        for k, (mask, sub) in enumerate(pieces)
    ]
    first_a, first_b, second_a, second_b, third = {}, {}, {}, {}, {}

    def spot_a(k, o, i):
        return got0.at[k, o * inner + i, pl.ds(0, quarter)]

    def spot_b(k, o, i):
        return got0.at[k, o * inner + i, pl.ds(quarter, quarter)]

    def stage_one(k):
        mask, sub = pieces[k]
        zeroth[k].wait_recv()
        first_a[k], first_b[k] = [], []
        for at_o, o in enumerate(outer_at + [mo]):
            for at_i, i in enumerate(inner_at + [mi]):
                t = o * inner + i
                add_rows(got0.at[k, t], got0.at[k, t], sums.at[line_of[mask], core, t, sub])
                if at_i < inner - 1:
                    first_a[k].append(
                        send(
                            spot_a(k, o, i), a1.at[k, at_i, o], sa1.at[k, at_i, at_o], ra1.at[k, at_i, at_o],
                            inner_peers[at_i],
                        )
                    )
                if at_o < outer - 1:
                    first_b[k].append(
                        send(
                            spot_b(k, o, i), b1.at[k, at_o, i], sb1.at[k, at_o, at_i], rb1.at[k, at_o, at_i],
                            outer_peers[at_o],
                        )
                    )

    def stage_two(k):
        for copy in first_a[k]:
            copy.wait_recv()
        second_a[k] = []
        for at_o, o in enumerate(outer_at + [mo]):
            mine = spot_a(k, o, mi)
            add_rows(mine, mine, *[a1.at[k, number, o] for number in range(inner - 1)])
            if at_o < outer - 1:
                second_a[k].append(
                    send(mine, a2.at[k, at_o], sa2.at[k, at_o], ra2.at[k, at_o], outer_peers[at_o])
                )
        for copy in first_b[k]:
            copy.wait_recv()
        second_b[k] = []
        for at_i, i in enumerate(inner_at + [mi]):
            mine = spot_b(k, mo, i)
            add_rows(mine, mine, *[b1.at[k, number, i] for number in range(outer - 1)])
            if at_i < inner - 1:
                second_b[k].append(
                    send(mine, b2.at[k, at_i], sb2.at[k, at_i], rb2.at[k, at_i], inner_peers[at_i])
                )

    def stage_three(k):
        mask, sub = pieces[k]
        for copy in second_a[k]:
            copy.wait_recv()
        add_rows(
            part.at[k, pl.ds(0, quarter)], spot_a(k, mo, mi), *[a2.at[k, number] for number in range(outer - 1)]
        )
        for copy in second_b[k]:
            copy.wait_recv()
        add_rows(
            part.at[k, pl.ds(quarter, quarter)], spot_b(k, mo, mi),
            *[b2.at[k, number] for number in range(inner - 1)],
        )
        if mask:
            third[mask, sub] = send(part.at[k], got2.at[k], s3.at[k], r3.at[k], line_peer[mask])

    run = subs * 2 * quarter // ROWS
    block = run * UPD
    unit = block // subs
    half_unit = unit // 2

    def spot(mask, source_time, sub):
        base = ((line_of[mask] * 2 + core) * times + source_time) * block + sub * unit
        return pl.multiple_of(base, SUB)

    from_line, near, far = {}, {}, {}

    def spread(mask, sub):
        place = table.at[pl.ds(spot(mask, time, sub), unit)]
        if mask:
            from_line[mask, sub].wait_recv()
            held = place
        else:
            held = upd.at[pl.ds(sub * unit, unit)]
        near[mask, sub] = [
            send(held, place, st.at[mask, sub, number], rt.at[mask, sub, number], peer)
            for number, peer in enumerate(inner_peers + outer_peers)
        ]

    def relay(mask, sub):
        far[mask, sub] = []
        number = inner + outer - 2
        for which, copy in enumerate(near[mask, sub]):
            copy.wait_recv()
            if which < inner - 1:
                origin = mo * inner + lax.rem(mi + inner - (which + 1), inner)
                rows, targets = 0, outer_peers
            else:
                origin = lax.rem(mo + outer - (which - inner + 2), outer) * inner + mi
                rows, targets = half_unit, inner_peers
            piece = table.at[pl.ds(pl.multiple_of(spot(mask, origin, sub) + rows, SUB), half_unit)]
            for peer in targets:
                far[mask, sub].append(
                    send(piece, piece, st.at[mask, sub, number], rt.at[mask, sub, number], peer)
                )
                number += 1

    def conclude(mask):
        for sub in range(subs):
            for copy in far[mask, sub]:
                copy.wait_recv()
        place = table.at[pl.ds(spot(mask, 0, 0), times * block)]
        return send(place, place, sd.at[mask], rd.at[mask], partner)

    def own_unit(sub):
        k = pieces.index((0, sub))
        for mask in masks:
            third[mask, sub].wait_recv()
        total = part.at[k]
        add_rows(total, total, *[got2.at[pieces.index((mask, sub))] for mask in masks])

        def solve(step, carry):
            base = step * SUB
            entry = [part[k, pl.ds(base * ROWS + row, SUB, stride=ROWS), :] for row in range(ROWS)]
            answer = damped_solve(entry[:15], entry[15:], 5, SOURCE_PAIRS)
            for c in range(UPD):
                upd[pl.ds(sub * unit + base * UPD + c, SUB, stride=UPD), :] = answer[c]
            return carry

        lax.fori_loop(0, run // subs // SUB, solve, 0)
        ordered = sorted(masks, key=lambda mask: (mask & (mask + 1) != 0, mask))
        for mask in ordered:
            from_line[mask, sub] = send(
                upd.at[pl.ds(sub * unit, unit)], table.at[pl.ds(spot(0, time, sub), unit)],
                su.at[mask, sub], ru.at[mask, sub], line_peer[mask],
            )
        spread(0, sub)
        table[pl.ds(spot(0, time, sub), unit), :] = upd[sub * unit : (sub + 1) * unit, :]

    groups = tiles // (2 * SUB)
    shares = 4
    for k in range(min(depth, count)):
        stage_one(k)
    for k in range(count):
        if k < shares:
            square_sums(weight, att, squares, groups * k // shares, groups * (k + 1) // shares)
        stage_two(k)
        if k + depth < count:
            stage_one(k + depth)
        if k > 0:
            stage_three(k - 1)
            if pieces[k - 1][0] == 0:
                own_unit(pieces[k - 1][1])
    stage_three(count - 1)
    own_unit(subs - 1)

    ordered = [0] + sorted(masks, key=lambda mask: (mask & (mask + 1) != 0, mask))
    sequence = [(mask, sub) for sub in range(subs) for mask in ordered]
    done = {(0, sub) for sub in range(subs)}
    relayed = []
    last = {}
    for at, item in enumerate(sequence):
        if item not in done:
            spread(*item)
        if at >= 2:
            relay(*sequence[at - 2])
            relayed.append(sequence[at - 2])
            if len(relayed) >= 2 and relayed[-2][1] == subs - 1:
                last[relayed[-2][0]] = conclude(relayed[-2][0])
    for item in sequence[-2:]:
        relay(*item)
    for mask in ordered:
        if mask not in last:
            last[mask] = conclude(mask)
    for mask in ordered:
        last[mask].wait_recv()
    for copy in pending:
        copy.wait_send()


def exchange(sums, obs_weight, attitude_partials):
    times, owners = lax.axis_size("tm"), lax.axis_size("sky")
    lines = owners // 2
    outer, inner = split_times(times)
    subs = 2
    total_rows = sums.shape[0]
    unit_rows = total_rows // (owners * times * subs)
    quarter = unit_rows // 2
    pixels = total_rows // ROWS
    block = pixels // (owners * times) * UPD
    tiles = obs_weight.shape[0]
    count = lines * subs
    dma = pltpu.SemaphoreType.DMA
    vmem = pltpu.VMEM
    near = inner + outer - 2
    far = 2 * (inner - 1) * (outer - 1)
    f32 = jnp.float32

    def pair(*shape):
        return [dma(shape), dma(shape)]

    return pl.pallas_call(
        functools.partial(exchange_kernel, times, lines, subs, 3),
        name="exchange",
        out_shape=(
            jax.ShapeDtypeStruct((pixels * UPD + SUB, LANES), f32),
            jax.ShapeDtypeStruct((tiles, LANES), f32),
        ),
        in_specs=[pl.BlockSpec(memory_space=pltpu.VMEM)] * 3,
        out_specs=(pl.BlockSpec(memory_space=pltpu.VMEM),) * 2,
        scratch_shapes=[
            vmem((count, times, unit_rows, LANES), f32),
            vmem((count, max(inner - 1, 1), outer, quarter, LANES), f32),
            vmem((count, max(outer - 1, 1), inner, quarter, LANES), f32),
            vmem((count, max(outer - 1, 1), quarter, LANES), f32),
            vmem((count, max(inner - 1, 1), quarter, LANES), f32),
            vmem((count, unit_rows, LANES), f32),
            vmem((count, unit_rows, LANES), f32),
            vmem((block, LANES), f32),
        ]
        + pair(count)
        + pair(count, max(inner - 1, 1), outer)
        + pair(count, max(outer - 1, 1), inner)
        + pair(count, max(outer - 1, 1))
        + pair(count, max(inner - 1, 1))
        + pair(count)
        + pair(lines, subs)
        + pair(lines, subs, near + far)
        + pair(lines),
        compiler_params=pltpu.CompilerParams(
            collective_id=0, has_side_effects=True, vmem_limit_bytes=24 * MIB
        ),
    )(sums.reshape(lines, 2, times, subs, unit_rows, LANES), obs_weight, attitude_partials)


def thirds(value):
    high = value.astype(jnp.bfloat16)
    rest = value - high.astype(jnp.float32)
    middle = rest.astype(jnp.bfloat16)
    return high, middle, (rest - middle.astype(jnp.float32)).astype(jnp.bfloat16)


def settle_kernel(
    times, owners, span, pixel_hbm, slot_hbm, knots, resid, weight, parts, att, index, table, squares,
    out, source_out, knot_out, pixel_ref, slot_ref, rows, terms, sums, before, mine, after, settles, values, others,
    sp, sl, sa, ra, sb, rb, sc, rc,
):
    mesh_ids = pl.DeviceIdType.MESH
    time, sky = lax.axis_index("tm"), lax.axis_index("sky")
    blocks = times * owners
    block = time * owners + sky
    nxt, prev = lax.rem(block + 1, blocks), lax.rem(block + blocks - 1, blocks)
    next_id, prev_id = (nxt // owners, lax.rem(nxt, owners)), (prev // owners, lax.rem(prev, owners))
    peers = [(time, lax.rem(sky + step, owners)) for step in range(1, owners)]
    barrier = pltpu.get_barrier_semaphore()
    for peer in [next_id, prev_id] + peers:
        pl.semaphore_signal(barrier, inc=1, device_id=peer, device_id_type=mesh_ids)

    pixels_in = pltpu.make_async_copy(pixel_hbm, pixel_ref, sp)
    slots_in = pltpu.make_async_copy(slot_hbm, slot_ref, sl)
    pixels_in.start()
    slots_in.start()
    pixels_in.wait()
    slots_in.wait()
    tiles = resid.shape[0]
    lane = lax.broadcasted_iota(jnp.int32, (SUB, LANES), 1)
    unroll = rows.shape[0]

    def group(step, carry):
        for part in range(unroll):
            base = pl.multiple_of((step * unroll + part) * SUB, SUB)
            here = pl.ds(base, SUB)
            for j in range(SUB):
                seat = slot_ref[pixel_ref[base + j]]
                rows[part, j * SUB : (j + 1) * SUB, :] = table[pl.ds(seat * UPD, SUB), :]
            ids = index[here, :]
            total = None
            for c in range(UPD):
                picked = jnp.take_along_axis(rows[part, pl.ds(c, SUB, stride=SUB), :], ids, axis=1)
                addend = parts[c, here, :] * picked
                total = addend if total is None else total + addend
            settled = resid[here, :] - total
            settles[here, :] = settled
            scaled = weight[here, :] * settled
            term = squares[here, :]
            for m in range(4):
                for c in range(4):
                    value = jnp.sum(scaled * att[4 * m + c, here, :], axis=1, keepdims=True)
                    term = jnp.where(lane == 16 * m + 10 + c, value, term)
            terms[here, :] = term
        return carry

    lax.fori_loop(0, tiles // (SUB * unroll), group, 0)
    knot = lax.broadcasted_iota(jnp.int32, (LANES, tiles), 0) + block * span
    hits = jnp.where(knot == knots[...], 1.0, 0.0).astype(jnp.bfloat16)
    placed = None
    for piece in thirds(terms[...]):
        got = jnp.dot(hits, piece, preferred_element_type=jnp.float32)
        placed = got if placed is None else placed + got
    turned = placed.T
    total = turned[:16]
    for m in range(1, 4):
        total = total + pltpu.roll(turned[16 * m : 16 * m + 16], m, 1)
    sums[...] = total

    pl.semaphore_wait(barrier, owners + 1)
    pending = []

    def send(source, target, send_sem, recv_sem, peer):
        copy = pltpu.make_async_remote_copy(
            src_ref=source, dst_ref=target, send_sem=send_sem, recv_sem=recv_sem,
            device_id=peer, device_id_type=mesh_ids,
        )
        copy.start()
        pending.append(copy)
        return copy

    handed = [send(sums, before, sa, ra, next_id), send(sums, after, sb, rb, prev_id)]
    per_owner = source_out.shape[1] // LANES

    def spread(step, carry):
        for part in range(SUB):
            pixel = step * SUB + part
            place = pl.ds(pl.multiple_of(pixel * LANES, LANES), LANES)
            source_out[:, place] = table[pl.ds((sky * per_owner + pixel) * UPD, UPD), :]
        return carry

    lax.fori_loop(0, per_owner // SUB, spread, 0)
    wide = lax.broadcasted_iota(jnp.int32, (16, LANES), 1)
    for copy in handed:
        copy.wait_recv()
    head = pltpu.roll(before[...], LANES - span, 1)
    tail = pltpu.roll(after[...], span, 1)
    whole = sums[...] + jnp.where((wide < 3) & (block > 0), head, 0.0)
    whole = whole + jnp.where((wide >= span) & (wide < span + 3), tail, 0.0)
    answer = damped_solve(
        [whole[n : n + 1] for n in range(10)], [whole[n : n + 1] for n in range(10, 14)], 4, KNOT_PAIRS
    )
    for c in range(4):
        mine[c : c + 1, :] = answer[c]
        mine[4 + c : 5 + c, :] = answer[c]
    around = [
        send(mine, others.at[sky], sc.at[number], rc.at[number], peer)
        for number, peer in enumerate(peers)
    ]
    others[pl.ds(sky, 1)] = mine[...][None]
    reach = jnp.where(block < blocks - 1, span + 3, span)
    extended = jnp.where(lane < reach, mine[...], 0.0)
    windows = []
    for m in range(0, 4, 2):
        low = extended if m == 0 else pltpu.roll(extended, LANES - m, 1)
        high = pltpu.roll(extended, LANES - m - 1, 1)
        half = lax.broadcasted_iota(jnp.int32, (SUB, LANES), 0) < 4
        windows.append(jnp.where(half, low, high))
    window = jnp.concatenate(windows, axis=0)
    picked = None
    for piece in thirds(window):
        got = jnp.dot(piece, hits, preferred_element_type=jnp.float32)
        picked = got if picked is None else picked + got
    for part in range(tiles // LANES):
        values[part * LANES : (part + 1) * LANES, :] = picked[:, part * LANES : (part + 1) * LANES].T

    def last(step, carry):
        for part in range(unroll):
            here = pl.ds(pl.multiple_of((step * unroll + part) * SUB, SUB), SUB)
            column = values[here, :]
            total = None
            for number in range(16):
                addend = att[number, here, :] * column[:, number : number + 1]
                total = addend if total is None else total + addend
            out[here, :] = settles[here, :] - total
        return carry

    lax.fori_loop(0, tiles // (SUB * unroll), last, 0)
    for copy in around:
        copy.wait_recv()
    each = LANES // span
    for first in range(0, owners, each):
        joined = jnp.where(lane < span, others[first], 0.0)
        for number in range(1, each):
            moved = pltpu.roll(others[first + number], number * span, 1)
            keep = (lane >= number * span) & (lane < (number + 1) * span)
            joined = jnp.where(keep, moved, joined)
        knot_out[:, first * span : first * span + LANES] = joined[:4]
    for copy in pending:
        copy.wait_send()


def settle(tile_pixel, pixel_slot, knots, residual, obs_weight, source_partials, attitude_partials, source_index, table, squares, span):
    times, owners = lax.axis_size("tm"), lax.axis_size("sky")
    tiles = residual.shape[0]
    unroll = 4
    pixels = pixel_slot.shape[0]
    dma = pltpu.SemaphoreType.DMA
    f32 = jnp.float32
    return pl.pallas_call(
        functools.partial(settle_kernel, times, owners, span),
        name="settle",
        out_shape=(
            jax.ShapeDtypeStruct(residual.shape, f32),
            jax.ShapeDtypeStruct((UPD, pixels // owners * LANES), f32),
            jax.ShapeDtypeStruct((4, span * owners), f32),
        ),
        in_specs=[pl.BlockSpec(memory_space=pltpu.HBM)] * 2 + [pl.BlockSpec(memory_space=pltpu.VMEM)] * 8,
        out_specs=(pl.BlockSpec(memory_space=pltpu.VMEM),) * 3,
        scratch_shapes=[
            pltpu.SMEM(tile_pixel.shape, jnp.int32),
            pltpu.SMEM(pixel_slot.shape, jnp.int32),
            pltpu.VMEM((unroll, SUB * SUB, LANES), f32),
            pltpu.VMEM((tiles, LANES), f32),
            pltpu.VMEM((16, LANES), f32),
            pltpu.VMEM((16, LANES), f32),
            pltpu.VMEM((SUB, LANES), f32),
            pltpu.VMEM((16, LANES), f32),
            pltpu.VMEM(residual.shape, f32),
            pltpu.VMEM((tiles, 16), f32),
            pltpu.VMEM((owners, SUB, LANES), f32),
            dma, dma, dma, dma, dma, dma, dma((owners - 1,)), dma((owners - 1,)),
        ],
        compiler_params=pltpu.CompilerParams(
            collective_id=1, has_side_effects=True, vmem_limit_bytes=24 * MIB
        ),
    )(tile_pixel, pixel_slot, knots, residual, obs_weight, source_partials, attitude_partials, source_index, table, squares)


def finish_kernel(*refs):
    count = (len(refs) - 1) // 2
    copies = [
        pltpu.make_async_copy(refs[number], refs[count + number], refs[-1].at[number]) for number in range(count)
    ]
    for copy in copies:
        copy.start()
    for copy in copies:
        copy.wait()


def finish(*results):
    return pl.pallas_call(
        finish_kernel,
        name="finish",
        out_shape=tuple(jax.ShapeDtypeStruct(value.shape, value.dtype) for value in results),
        in_specs=[pl.BlockSpec(memory_space=pltpu.VMEM)] * len(results),
        out_specs=(pl.BlockSpec(memory_space=pltpu.HBM),) * len(results),
        scratch_shapes=[pltpu.SemaphoreType.DMA((len(results),))],
        compiler_params=pltpu.CompilerParams(vmem_limit_bytes=8 * MIB),
    )(*results)


def body(residual, obs_weight, source_partials, attitude_partials, source_index, tile_pixel, tile_knot, pixel_slot):
    span = KNOTS_DEV // lax.axis_size("sky")
    sums = local_sums(tile_pixel, pixel_slot, residual, obs_weight, source_partials, source_index)
    table, squares = exchange(sums, obs_weight, attitude_partials)
    results = settle(
        tile_pixel, pixel_slot, tile_knot[None, :], residual, obs_weight, source_partials,
        attitude_partials, source_index, table, squares, span,
    )
    return finish(*results)


def solution(mesh):
    in_specs = (
        P(("tm", "sky"), None),
        P(("tm", "sky"), None),
        P(None, ("tm", "sky"), None),
        P(None, ("tm", "sky"), None),
        P(("tm", "sky"), None),
        P(("tm", "sky")),
        P(("tm", "sky")),
        P(),
    )
    out_specs = (P(("tm", "sky"), None), P(None, "sky"), P(None, "tm"))
    return jax.shard_map(body, mesh=mesh, in_specs=in_specs, out_specs=out_specs, check_vma=False)
```

```python
import functools

import jax
import jax.numpy as jnp
from jax import lax
from jax.experimental import pallas as pl
from jax.experimental.pallas import tpu as pltpu
from jax.sharding import PartitionSpec as P

KNOTS_DEV = 512
ROWS = 20
PAD = 24
UPD = 5
LANES = 128
SUB = 8
MIB = 1024 * 1024

SOURCE_PAIRS = tuple(((first, second) for first in range(5) for second in range(first, 5)))
KNOT_PAIRS = tuple(((first, second) for first in range(4) for second in range(first, 4)))


def damped_solve(normal, target, order, pairs):
    entries = {}
    for number, couple in enumerate(pairs):
        entries[couple] = normal[number]
    factor = {}
    for column in range(order):
        pivot_value = entries[column, column] + 1.0
        for earlier in range(column):
            pivot_value = pivot_value - factor[column, earlier] * factor[column, earlier]
        pivot_value = jnp.sqrt(pivot_value)
        factor[column, column] = pivot_value
        for below in range(column + 1, order):
            current = entries[column, below]
            for earlier in range(column):
                current = current - factor[below, earlier] * factor[column, earlier]
            factor[below, column] = current / pivot_value
    forward = []
    for column in range(order):
        current = target[column]
        for earlier in range(column):
            current = current - factor[column, earlier] * forward[earlier]
        forward.append(current / factor[column, column])
    answer = [None] * order
    for column in reversed(range(order)):
        current = forward[column]
        for later in range(column + 1, order):
            current = current - factor[later, column] * answer[later]
        answer[column] = current / factor[column, column]
    return answer


def split_times(times):
    inner = 2 if times % 2 == 0 else 1
    return times // inner, inner


def sums_kernel(
    tiles_step, pixel_hbm, slot_hbm, resid_hbm, weight_hbm, parts_hbm, index_hbm, out,
    pixel_ref, slot_ref, resid, weight, parts, index, stage, prods, sems,
):
    copies = [
        pltpu.make_async_copy(source, target, sems.at[number])
        for number, (source, target) in enumerate(
            [
                (pixel_hbm, pixel_ref),
                (slot_hbm, slot_ref),
                (resid_hbm, resid),
                (weight_hbm, weight),
                (parts_hbm, parts),
                (index_hbm, index),
            ]
        )
    ]
    for copy in copies:
        copy.start()
    tiles = resid.shape[0]
    zero = jnp.zeros((256, LANES), jnp.float32)

    def clear(step, carry):
        out[pl.ds(pl.multiple_of(step * 256, 256), 256), :] = zero
        return carry

    lax.fori_loop(0, out.shape[0] // 256, clear, 0)
    stage[...] = jnp.zeros_like(stage)
    sources = lax.broadcasted_iota(jnp.int32, (SUB, LANES), 0).astype(jnp.float32)
    bands = [
        jnp.concatenate([sources + float(16 * band), sources + float(16 * band + 8)], axis=0).astype(jnp.bfloat16)
        for band in range(LANES // 16)
    ]
    lanes_of = jnp.concatenate(bands, axis=0)
    one = jnp.ones((LANES, LANES), jnp.bfloat16)
    none = jnp.zeros((LANES, LANES), jnp.bfloat16)
    blank = jnp.zeros((2 * PAD, LANES), jnp.bfloat16)
    for copy in copies:
        copy.wait()

    def accumulate(step, slot):
        for j in range(tiles_step):
            start = slot_ref[pixel_ref[step * tiles_step + j]] * ROWS
            values = prods[pl.ds(slot * tiles_step * PAD + j * PAD, PAD), :]
            out[pl.ds(start, ROWS), :] += values[:ROWS]

    def multiply(step, slot):
        for part in range(tiles_step // SUB):
            base = pl.multiple_of(step * tiles_step + part * SUB, SUB)
            here = pl.ds(base, SUB)
            fields = [parts[c, here, :] for c in range(5)]
            scaled = [weight[here, :] * field for field in fields]
            baseline = resid[here, :]
            row = part * SUB * PAD
            for first, second in SOURCE_PAIRS:
                stage[pl.ds(row, SUB, stride=PAD), :] = scaled[first] * fields[second]
                row += 1
            for first in range(5):
                stage[pl.ds(row, SUB, stride=PAD), :] = scaled[first] * baseline
                row += 1
            ids = index[here, :].astype(jnp.float32)
            for j in range(0, SUB, 2):
                row = (part * SUB + j) * PAD
                lhs, hits = [], []
                for side in range(2):
                    values = stage[row + side * PAD : row + (side + 1) * PAD, :]
                    high = values.astype(jnp.bfloat16).astype(jnp.float32)
                    both = jnp.concatenate([high, values - high], axis=0).astype(jnp.bfloat16)
                    lhs.append(jnp.concatenate([both, blank] if side == 0 else [blank, both], axis=1))
                    wide = jnp.broadcast_to(ids[j + side : j + side + 1, :], (16, LANES)).astype(jnp.bfloat16)
                    tall = jnp.concatenate([wide] * (LANES // 16), axis=0)
                    hits.append(jnp.where(lanes_of == tall, one, none))
                got = lax.dot_general(
                    jnp.concatenate(lhs, axis=0),
                    jnp.concatenate(hits, axis=1),
                    (((1,), (1,)), ((), ())),
                    preferred_element_type=jnp.float32,
                )
                for side in range(2):
                    low = 2 * side * PAD
                    prods[pl.ds(slot * tiles_step * PAD + row + side * PAD, PAD), :] = (
                        got[low : low + PAD] + got[low + PAD : low + 2 * PAD]
                    )

    steps = tiles // tiles_step
    multiply(0, 0)

    def pair(step, carry):
        multiply(2 * step + 1, 1)
        accumulate(2 * step, 0)
        multiply(jnp.minimum(2 * step + 2, steps - 1), 0)
        accumulate(2 * step + 1, 1)
        return carry

    lax.fori_loop(0, steps // 2, pair, 0)


def local_sums(tile_pixel, pixel_slot, residual, obs_weight, source_partials, source_index):
    pixels = pixel_slot.shape[0]
    tiles_step = 16
    return pl.pallas_call(
        functools.partial(sums_kernel, tiles_step),
        name="local_sums",
        out_shape=jax.ShapeDtypeStruct((pixels * ROWS, LANES), jnp.float32),
        in_specs=[pl.BlockSpec(memory_space=pltpu.HBM)] * 6,
        out_specs=pl.BlockSpec(memory_space=pltpu.VMEM),
        scratch_shapes=[
            pltpu.SMEM(tile_pixel.shape, jnp.int32),
            pltpu.SMEM(pixel_slot.shape, jnp.int32),
            pltpu.VMEM(residual.shape, jnp.float32),
            pltpu.VMEM(obs_weight.shape, jnp.float32),
            pltpu.VMEM(source_partials.shape, jnp.float32),
            pltpu.VMEM(source_index.shape, jnp.int32),
            pltpu.VMEM((tiles_step * PAD, LANES), jnp.float32),
            pltpu.VMEM((2 * tiles_step * PAD, LANES), jnp.float32),
            pltpu.SemaphoreType.DMA((6,)),
        ],
        compiler_params=pltpu.CompilerParams(vmem_limit_bytes=18 * MIB),
    )(*[pltpu.with_memory_space_constraint(v, pltpu.HBM) for v in (tile_pixel, pixel_slot, residual, obs_weight, source_partials, source_index)])


def add_rows(target, *sources):
    rows = target.shape[0]
    step_rows = next(size for size in range(160, 0, -SUB) if rows % size == 0)

    def one(step, carry):
        here = pl.ds(pl.multiple_of(step * step_rows, step_rows), step_rows)
        total = sources[0][here, :]
        for source in sources[1:]:
            total = total + source[here, :]
        target[here, :] = total
        return carry

    lax.fori_loop(0, rows // step_rows, one, 0)


def square_sums(weight, att, rows, first, last):
    lane = lax.broadcasted_iota(jnp.int32, (SUB, LANES), 1)

    def group(step, carry):
        for part in range(2):
            here = pl.ds(pl.multiple_of(step * 2 * SUB + part * SUB, SUB), SUB)
            scale = weight[here, :]
            total = jnp.zeros((SUB, LANES), jnp.float32)
            for m in range(4):
                fields = [att[4 * m + c, here, :] for c in range(4)]
                scaled = [scale * field for field in fields]
                for number, (a, b) in enumerate(KNOT_PAIRS):
                    value = jnp.sum(scaled[a] * fields[b], axis=1, keepdims=True)
                    total = jnp.where(lane == 16 * m + number, value, total)
            rows[here, :] = total
        return carry

    lax.fori_loop(first, last, group, 0)


def exchange_kernel(
    times, lines, subs, units, depth, far_rows, sums, weight, att, table, squares,
    got0, gotz, gz2, a1, b1, a2, b2, part, got2, mine, upd, *sems
):
    (
        s0, r0, sz, rz, sy, ry, sa1, ra1, sb1, rb1, sa2, ra2, sb2, rb2, s3, r3, su, ru, st, rt, sd, rd,
    ) = sems
    outer, inner = split_times(times)
    mesh_ids = pl.DeviceIdType.MESH
    time, sky = lax.axis_index("tm"), lax.axis_index("sky")
    line, core = sky // 2, sky % 2
    mo, mi = time // inner, time % inner
    partner = (time, sky + 1 - 2 * core)
    tiles = weight.shape[0]
    rows = got0.shape[2]
    inner_at = [lax.rem(mi + step, inner) for step in range(1, inner)]
    outer_at = [lax.rem(mo + step, outer) for step in range(1, outer)]
    inner_peers = [(mo * inner + i, sky) for i in inner_at]
    outer_peers = [(o * inner + mi, sky) for o in outer_at]
    odd = [mask for mask in range(lines - 1, 1, -1) if mask % 2]
    even = [mask for mask in range(lines - 1, 0, -1) if mask % 2 == 0]
    masks = odd + even + ([1] if lines > 1 else [])
    direct = [mask for mask in masks if mask not in odd]
    line_of = {mask: jnp.bitwise_xor(line, mask) for mask in range(lines)}
    line_peer = {mask: (time, line_of[mask] * 2 + core) for mask in direct}

    barrier = pltpu.get_barrier_semaphore()
    peers = [partner] + inner_peers + outer_peers + [line_peer[mask] for mask in direct]
    for peer in peers:
        pl.semaphore_signal(barrier, inc=1, device_id=peer, device_id_type=mesh_ids)
    pl.semaphore_wait(barrier, len(peers))

    pending = []

    def send(source, target, send_sem, recv_sem, peer):
        copy = pltpu.make_async_remote_copy(
            src_ref=source, dst_ref=target, send_sem=send_sem, recv_sem=recv_sem,
            device_id=peer, device_id_type=mesh_ids,
        )
        copy.start()
        pending.append(copy)
        return copy

    pieces = [(mask, sub) for mask in masks + [0] for sub in range(subs)]
    count = len(pieces)
    zeroth, far_zeroth, far_third = {}, {}, {}
    far_at = pl.ds(subs * rows, far_rows)

    def stage_zero(k):
        mask, sub = pieces[k]
        zeroth[k] = send(
            sums.at[line_of[mask], 1 - core, :, pl.ds(sub * rows, rows)], got0.at[k], s0.at[k], r0.at[k], partner
        )

    def far_zero(mask):
        far_zeroth[mask] = send(
            sums.at[line_of[mask], 1 - core, :, far_at], gotz.at[mask], sz.at[mask], rz.at[mask], partner
        )

    far_order = masks + [0]
    for k in range(max(count, lines)):
        if k < count:
            stage_zero(k)
        if k < lines:
            far_zero(far_order[k])

    def far_add(mask):
        far_zeroth[mask].wait_recv()
        for t in range(times):
            add_rows(gotz.at[mask, t], gotz.at[mask, t], sums.at[line_of[mask], core, t, far_at])

    def far_send(mask):
        if mask in even and mask + 1 < lines:
            far_third[mask + 1].wait_recv()
            for t in range(times):
                add_rows(gotz.at[mask, t], gotz.at[mask, t], gz2.at[mask + 1, t])
        peer = line_peer[mask if mask in direct else 1]
        far_third[mask] = send(gotz.at[mask], gz2.at[mask], sy.at[mask], ry.at[mask], peer)

    def far_close():
        for mask in direct:
            far_third[mask].wait_recv()
        for t in range(times):
            add_rows(gotz.at[0, t], gotz.at[0, t], *[gz2.at[mask, t] for mask in direct])

    first_a, first_b, second_a, second_b, third = {}, {}, {}, {}, {}

    def held(k):
        return (got0.at[k], rows // 2) if k < count else (gotz.at[0], far_rows // 2)

    def spot_a(k, o, i):
        ref, quarter = held(k)
        return ref.at[o * inner + i, pl.ds(0, quarter)]

    def spot_b(k, o, i):
        ref, quarter = held(k)
        return ref.at[o * inner + i, pl.ds(quarter, quarter)]

    def stage_one(k):
        quarter = held(k)[1]
        size = pl.ds(0, quarter)
        if k < count:
            mask, sub = pieces[k]
            zeroth[k].wait_recv()
        else:
            far_close()
        first_a[k], first_b[k] = [], []
        for at_o, o in enumerate(outer_at + [mo]):
            for at_i, i in enumerate(inner_at + [mi]):
                t = o * inner + i
                if k < count:
                    add_rows(
                        got0.at[k, t], got0.at[k, t],
                        sums.at[line_of[mask], core, t, pl.ds(sub * rows, rows)],
                    )
                if at_i < inner - 1:
                    first_a[k].append(
                        send(
                            spot_a(k, o, i), a1.at[k, at_i, o, size], sa1.at[k, at_i, at_o],
                            ra1.at[k, at_i, at_o], inner_peers[at_i],
                        )
                    )
                if at_o < outer - 1:
                    first_b[k].append(
                        send(
                            spot_b(k, o, i), b1.at[k, at_o, i, size], sb1.at[k, at_o, at_i],
                            rb1.at[k, at_o, at_i], outer_peers[at_o],
                        )
                    )

    def stage_two(k):
        size = pl.ds(0, held(k)[1])
        for copy in first_a[k]:
            copy.wait_recv()
        second_a[k] = []
        for at_o, o in enumerate(outer_at + [mo]):
            own = spot_a(k, o, mi)
            add_rows(own, own, *[a1.at[k, number, o, size] for number in range(inner - 1)])
            if at_o < outer - 1:
                second_a[k].append(
                    send(own, a2.at[k, at_o, size], sa2.at[k, at_o], ra2.at[k, at_o], outer_peers[at_o])
                )
        for copy in first_b[k]:
            copy.wait_recv()
        second_b[k] = []
        for at_i, i in enumerate(inner_at + [mi]):
            own = spot_b(k, mo, i)
            add_rows(own, own, *[b1.at[k, number, i, size] for number in range(outer - 1)])
            if at_i < inner - 1:
                second_b[k].append(
                    send(own, b2.at[k, at_i, size], sb2.at[k, at_i], rb2.at[k, at_i], inner_peers[at_i])
                )

    def stage_three(k):
        quarter = held(k)[1]
        size = pl.ds(0, quarter)
        if k >= count:
            mask, sub, target, base = 0, subs, mine, subs * rows
        elif pieces[k][0]:
            (mask, sub), target, base = pieces[k], part.at[k], 0
        else:
            (mask, sub), target, base = pieces[k], mine, pieces[k][1] * rows
        extra = []
        if mask in even and mask + 1 < lines:
            third[mask + 1, sub].wait_recv()
            extra = [got2.at[pieces.index((mask + 1, sub))]]
        elif mask == 0 and k < count:
            for other in direct:
                third[other, sub].wait_recv()
            extra = [got2.at[pieces.index((other, sub))] for other in direct]
        for copy in second_a[k]:
            copy.wait_recv()
        add_rows(
            target.at[pl.ds(base, quarter)], spot_a(k, mo, mi),
            *[a2.at[k, number, size] for number in range(outer - 1)],
            *[ref.at[size] for ref in extra],
        )
        for copy in second_b[k]:
            copy.wait_recv()
        add_rows(
            target.at[pl.ds(base + quarter, quarter)], spot_b(k, mo, mi),
            *[b2.at[k, number, size] for number in range(inner - 1)],
            *[ref.at[pl.ds(quarter, quarter)] for ref in extra],
        )
        if mask:
            peer = line_peer[mask if mask in direct else 1]
            third[mask, sub] = send(part.at[k], got2.at[k], s3.at[k], r3.at[k], peer)

    groups = tiles // (2 * SUB)
    shares = 4
    total = count + 1
    for at in range(depth):
        stage_one(at)
        far_add(far_order[at])
        if far_order[at] in odd or far_order[at] == 1:
            far_send(far_order[at])
    waiting = [mask for mask in far_order[depth:]]
    late = [mask for mask in far_order[:depth] if mask in even]
    for k in range(total):
        if k < shares:
            square_sums(weight, att, squares, groups * k // shares, groups * (k + 1) // shares)
        stage_two(k)
        if k + depth < total:
            stage_one(k + depth)
        if waiting and k < depth:
            for mask in waiting:
                far_add(mask)
                if mask in odd or mask == 1:
                    far_send(mask)
                elif mask in even:
                    late.append(mask)
            waiting = []
        elif late:
            for mask in late:
                far_send(mask)
            late = []
        if k > 0:
            stage_three(k - 1)
    stage_three(total - 1)

    run = mine.shape[0] // ROWS
    block = run * UPD
    unit = block // units
    half_unit = unit // 2

    def spot(mask, source_time, sub):
        base = ((line_of[mask] * 2 + core) * times + source_time) * block + sub * unit
        return pl.multiple_of(base, SUB)

    from_line, near, far = {}, {}, {}

    def spread(mask, sub):
        place = table.at[pl.ds(spot(mask, time, sub), unit)]
        held_in = place
        if mask:
            from_line[mask, sub].wait_recv()
            if mask in even and mask + 1 < lines:
                from_line[mask + 1, sub] = send(
                    place, place, su.at[mask + 1, sub], ru.at[mask + 1, sub], line_peer[1]
                )
        else:
            held_in = upd.at[pl.ds(sub * unit, unit)]
        near[mask, sub] = [
            send(held_in, place, st.at[mask, sub, number], rt.at[mask, sub, number], peer)
            for number, peer in enumerate(inner_peers + outer_peers)
        ]

    def relay(mask, sub):
        far[mask, sub] = []
        number = inner + outer - 2
        for which, copy in enumerate(near[mask, sub]):
            copy.wait_recv()
            if which < inner - 1:
                origin = mo * inner + lax.rem(mi + inner - (which + 1), inner)
                start, targets = 0, outer_peers
            else:
                origin = lax.rem(mo + outer - (which - inner + 2), outer) * inner + mi
                start, targets = half_unit, inner_peers
            piece = table.at[pl.ds(pl.multiple_of(spot(mask, origin, sub) + start, SUB), half_unit)]
            for peer in targets:
                far[mask, sub].append(
                    send(piece, piece, st.at[mask, sub, number], rt.at[mask, sub, number], peer)
                )
                number += 1

    def conclude(mask):
        for sub in range(units):
            for copy in far[mask, sub]:
                copy.wait_recv()
        place = table.at[pl.ds(spot(mask, 0, 0), times * block)]
        return send(place, place, sd.at[mask], rd.at[mask], partner)

    for sub in range(units):
        pixels = run // units

        def solve(step, carry):
            base = sub * pixels + step * SUB
            entry = [mine[pl.ds(base * ROWS + row, SUB, stride=ROWS), :] for row in range(ROWS)]
            answer = damped_solve(entry[:15], entry[15:], 5, SOURCE_PAIRS)
            for c in range(UPD):
                upd[pl.ds(base * UPD + c, SUB, stride=UPD), :] = answer[c]
            return carry

        lax.fori_loop(0, pixels // SUB, solve, 0)
        for mask in even + [1]:
            from_line[mask, sub] = send(
                upd.at[pl.ds(sub * unit, unit)], table.at[pl.ds(spot(0, time, sub), unit)],
                su.at[mask, sub], ru.at[mask, sub], line_peer[mask],
            )
        spread(0, sub)
        table[pl.ds(spot(0, time, sub), unit), :] = upd[sub * unit : (sub + 1) * unit, :]

    ordered = [0, 1] + even[::-1] + odd[::-1]
    sequence = [(mask, sub) for mask in ordered for sub in range(units)]
    last = {}
    for at, item in enumerate(sequence):
        if item[0]:
            spread(*item)
        if at >= 2:
            relay(*sequence[at - 2])
        if at >= 3 and sequence[at - 3][1] == units - 1:
            last[sequence[at - 3][0]] = conclude(sequence[at - 3][0])
    for item in sequence[-2:]:
        relay(*item)
    for mask in ordered:
        if mask not in last:
            last[mask] = conclude(mask)
    for mask in ordered:
        last[mask].wait_recv()
    for copy in pending:
        copy.wait_send()


def exchange(sums, obs_weight, attitude_partials):
    times, owners = lax.axis_size("tm"), lax.axis_size("sky")
    lines = owners // 2
    outer, inner = split_times(times)
    total_rows = sums.shape[0]
    chunk = total_rows // (owners * times)
    pixels = total_rows // ROWS
    block = chunk // ROWS * UPD
    far_rows = chunk // 4
    rest = chunk - far_rows
    subs = 2 if rest % 32 == 0 else 1
    units = 2 if block % 32 == 0 else 1
    rows = rest // subs
    quarter = max(rows, far_rows) // 2
    tiles = obs_weight.shape[0]
    count = lines * subs
    total = count + 1
    dma = pltpu.SemaphoreType.DMA
    vmem = pltpu.VMEM
    near = inner + outer - 2
    far = 2 * (inner - 1) * (outer - 1)
    f32 = jnp.float32

    def pair(*shape):
        return [dma(shape), dma(shape)]

    return pl.pallas_call(
        functools.partial(exchange_kernel, times, lines, subs, units, 2, far_rows),
        name="exchange",
        out_shape=(
            jax.ShapeDtypeStruct((pixels * UPD + SUB, LANES), f32),
            jax.ShapeDtypeStruct((tiles, LANES), f32),
        ),
        in_specs=[pl.BlockSpec(memory_space=pltpu.VMEM)] * 3,
        out_specs=(pl.BlockSpec(memory_space=pltpu.VMEM),) * 2,
        scratch_shapes=[
            vmem((count, times, rows, LANES), f32),
            vmem((lines, times, far_rows, LANES), f32),
            vmem((lines, times, far_rows, LANES), f32),
            vmem((total, max(inner - 1, 1), outer, quarter, LANES), f32),
            vmem((total, max(outer - 1, 1), inner, quarter, LANES), f32),
            vmem((total, max(outer - 1, 1), quarter, LANES), f32),
            vmem((total, max(inner - 1, 1), quarter, LANES), f32),
            vmem((count, rows, LANES), f32),
            vmem((count, rows, LANES), f32),
            vmem((chunk, LANES), f32),
            vmem((block, LANES), f32),
        ]
        + pair(count)
        + pair(lines)
        + pair(lines)
        + pair(total, max(inner - 1, 1), outer)
        + pair(total, max(outer - 1, 1), inner)
        + pair(total, max(outer - 1, 1))
        + pair(total, max(inner - 1, 1))
        + pair(count)
        + pair(lines, units)
        + pair(lines, units, near + far)
        + pair(lines),
        compiler_params=pltpu.CompilerParams(
            collective_id=0, has_side_effects=True, vmem_limit_bytes=24 * MIB
        ),
    )(sums.reshape(lines, 2, times, chunk, LANES), obs_weight, attitude_partials)


def thirds(value):
    high = value.astype(jnp.bfloat16)
    rest = value - high.astype(jnp.float32)
    middle = rest.astype(jnp.bfloat16)
    return high, middle, (rest - middle.astype(jnp.float32)).astype(jnp.bfloat16)


def settle_kernel(
    times, owners, span, pixel_hbm, slot_hbm, knots, resid, weight, parts, att, index, table, squares,
    out, source_out, knot_out, pixel_ref, slot_ref, rows, terms, sums, before, mine, after, settles, values, others,
    sp, sl, sa, ra, sb, rb, sc, rc,
):
    mesh_ids = pl.DeviceIdType.MESH
    time, sky = lax.axis_index("tm"), lax.axis_index("sky")
    blocks = times * owners
    block = time * owners + sky
    nxt, prev = lax.rem(block + 1, blocks), lax.rem(block + blocks - 1, blocks)
    next_id, prev_id = (nxt // owners, lax.rem(nxt, owners)), (prev // owners, lax.rem(prev, owners))
    peers = [(time, lax.rem(sky + step, owners)) for step in range(1, owners)]
    barrier = pltpu.get_barrier_semaphore()
    for peer in [next_id, prev_id] + peers:
        pl.semaphore_signal(barrier, inc=1, device_id=peer, device_id_type=mesh_ids)

    pixels_in = pltpu.make_async_copy(pixel_hbm, pixel_ref, sp)
    slots_in = pltpu.make_async_copy(slot_hbm, slot_ref, sl)
    pixels_in.start()
    slots_in.start()
    pixels_in.wait()
    slots_in.wait()
    tiles = resid.shape[0]
    lane = lax.broadcasted_iota(jnp.int32, (SUB, LANES), 1)
    unroll = rows.shape[0]

    def group(step, carry):
        for part in range(unroll):
            base = pl.multiple_of((step * unroll + part) * SUB, SUB)
            here = pl.ds(base, SUB)
            for j in range(SUB):
                seat = slot_ref[pixel_ref[base + j]]
                rows[part, j * SUB : (j + 1) * SUB, :] = table[pl.ds(seat * UPD, SUB), :]
            ids = index[here, :]
            total = None
            for c in range(UPD):
                picked = jnp.take_along_axis(rows[part, pl.ds(c, SUB, stride=SUB), :], ids, axis=1)
                addend = parts[c, here, :] * picked
                total = addend if total is None else total + addend
            settled = resid[here, :] - total
            settles[here, :] = settled
            scaled = weight[here, :] * settled
            term = squares[here, :]
            for m in range(4):
                for c in range(4):
                    value = jnp.sum(scaled * att[4 * m + c, here, :], axis=1, keepdims=True)
                    term = jnp.where(lane == 16 * m + 10 + c, value, term)
            terms[here, :] = term
        return carry

    lax.fori_loop(0, tiles // (SUB * unroll), group, 0)
    knot = lax.broadcasted_iota(jnp.int32, (LANES, tiles), 0) + block * span
    hits = jnp.where(knot == knots[...], 1.0, 0.0).astype(jnp.bfloat16)
    placed = None
    for piece in thirds(terms[...]):
        got = jnp.dot(hits, piece, preferred_element_type=jnp.float32)
        placed = got if placed is None else placed + got
    turned = placed.T
    total = turned[:16]
    for m in range(1, 4):
        total = total + pltpu.roll(turned[16 * m : 16 * m + 16], m, 1)
    sums[...] = total

    pl.semaphore_wait(barrier, owners + 1)
    pending = []

    def send(source, target, send_sem, recv_sem, peer):
        copy = pltpu.make_async_remote_copy(
            src_ref=source, dst_ref=target, send_sem=send_sem, recv_sem=recv_sem,
            device_id=peer, device_id_type=mesh_ids,
        )
        copy.start()
        pending.append(copy)
        return copy

    handed = [send(sums, before, sa, ra, next_id), send(sums, after, sb, rb, prev_id)]
    per_owner = source_out.shape[1] // LANES

    def spread(step, carry):
        for part in range(SUB):
            pixel = step * SUB + part
            place = pl.ds(pl.multiple_of(pixel * LANES, LANES), LANES)
            source_out[:, place] = table[pl.ds((sky * per_owner + pixel) * UPD, UPD), :]
        return carry

    lax.fori_loop(0, per_owner // SUB, spread, 0)
    wide = lax.broadcasted_iota(jnp.int32, (16, LANES), 1)
    for copy in handed:
        copy.wait_recv()
    head = pltpu.roll(before[...], LANES - span, 1)
    tail = pltpu.roll(after[...], span, 1)
    whole = sums[...] + jnp.where((wide < 3) & (block > 0), head, 0.0)
    whole = whole + jnp.where((wide >= span) & (wide < span + 3), tail, 0.0)
    answer = damped_solve(
        [whole[n : n + 1] for n in range(10)], [whole[n : n + 1] for n in range(10, 14)], 4, KNOT_PAIRS
    )
    for c in range(4):
        mine[c : c + 1, :] = answer[c]
        mine[4 + c : 5 + c, :] = answer[c]
    around = [
        send(mine, others.at[sky], sc.at[number], rc.at[number], peer)
        for number, peer in enumerate(peers)
    ]
    others[pl.ds(sky, 1)] = mine[...][None]
    reach = jnp.where(block < blocks - 1, span + 3, span)
    extended = jnp.where(lane < reach, mine[...], 0.0)
    windows = []
    for m in range(0, 4, 2):
        low = extended if m == 0 else pltpu.roll(extended, LANES - m, 1)
        high = pltpu.roll(extended, LANES - m - 1, 1)
        half = lax.broadcasted_iota(jnp.int32, (SUB, LANES), 0) < 4
        windows.append(jnp.where(half, low, high))
    window = jnp.concatenate(windows, axis=0)
    picked = None
    for piece in thirds(window):
        got = jnp.dot(piece, hits, preferred_element_type=jnp.float32)
        picked = got if picked is None else picked + got
    for part in range(tiles // LANES):
        values[part * LANES : (part + 1) * LANES, :] = picked[:, part * LANES : (part + 1) * LANES].T

    def last(step, carry):
        for part in range(unroll):
            here = pl.ds(pl.multiple_of((step * unroll + part) * SUB, SUB), SUB)
            column = values[here, :]
            total = None
            for number in range(16):
                addend = att[number, here, :] * column[:, number : number + 1]
                total = addend if total is None else total + addend
            out[here, :] = settles[here, :] - total
        return carry

    lax.fori_loop(0, tiles // (SUB * unroll), last, 0)
    for copy in around:
        copy.wait_recv()
    each = LANES // span
    for first in range(0, owners, each):
        joined = jnp.where(lane < span, others[first], 0.0)
        for number in range(1, each):
            moved = pltpu.roll(others[first + number], number * span, 1)
            keep = (lane >= number * span) & (lane < (number + 1) * span)
            joined = jnp.where(keep, moved, joined)
        knot_out[:, first * span : first * span + LANES] = joined[:4]
    for copy in pending:
        copy.wait_send()


def settle(tile_pixel, pixel_slot, knots, residual, obs_weight, source_partials, attitude_partials, source_index, table, squares, span):
    times, owners = lax.axis_size("tm"), lax.axis_size("sky")
    tiles = residual.shape[0]
    unroll = 8
    pixels = pixel_slot.shape[0]
    dma = pltpu.SemaphoreType.DMA
    f32 = jnp.float32
    return pl.pallas_call(
        functools.partial(settle_kernel, times, owners, span),
        name="settle",
        out_shape=(
            jax.ShapeDtypeStruct(residual.shape, f32),
            jax.ShapeDtypeStruct((UPD, pixels // owners * LANES), f32),
            jax.ShapeDtypeStruct((4, span * owners), f32),
        ),
        in_specs=[pl.BlockSpec(memory_space=pltpu.HBM)] * 2 + [pl.BlockSpec(memory_space=pltpu.VMEM)] * 8,
        out_specs=(pl.BlockSpec(memory_space=pltpu.VMEM),) * 3,
        scratch_shapes=[
            pltpu.SMEM(tile_pixel.shape, jnp.int32),
            pltpu.SMEM(pixel_slot.shape, jnp.int32),
            pltpu.VMEM((unroll, SUB * SUB, LANES), f32),
            pltpu.VMEM((tiles, LANES), f32),
            pltpu.VMEM((16, LANES), f32),
            pltpu.VMEM((16, LANES), f32),
            pltpu.VMEM((SUB, LANES), f32),
            pltpu.VMEM((16, LANES), f32),
            pltpu.VMEM(residual.shape, f32),
            pltpu.VMEM((tiles, 16), f32),
            pltpu.VMEM((owners, SUB, LANES), f32),
            dma, dma, dma, dma, dma, dma, dma((owners - 1,)), dma((owners - 1,)),
        ],
        compiler_params=pltpu.CompilerParams(
            collective_id=1, has_side_effects=True, vmem_limit_bytes=24 * MIB
        ),
    )(tile_pixel, pixel_slot, knots, residual, obs_weight, source_partials, attitude_partials, source_index, table, squares)


def finish_kernel(*refs):
    count = (len(refs) - 1) // 2
    copies = [
        pltpu.make_async_copy(refs[number], refs[count + number], refs[-1].at[number]) for number in range(count)
    ]
    for copy in copies:
        copy.start()
    for copy in copies:
        copy.wait()


def finish(*results):
    return pl.pallas_call(
        finish_kernel,
        name="finish",
        out_shape=tuple(jax.ShapeDtypeStruct(value.shape, value.dtype) for value in results),
        in_specs=[pl.BlockSpec(memory_space=pltpu.VMEM)] * len(results),
        out_specs=(pl.BlockSpec(memory_space=pltpu.HBM),) * len(results),
        scratch_shapes=[pltpu.SemaphoreType.DMA((len(results),))],
        compiler_params=pltpu.CompilerParams(vmem_limit_bytes=8 * MIB),
    )(*results)


def body(residual, obs_weight, source_partials, attitude_partials, source_index, tile_pixel, tile_knot, pixel_slot):
    span = KNOTS_DEV // lax.axis_size("sky")
    sums = local_sums(tile_pixel, pixel_slot, residual, obs_weight, source_partials, source_index)
    table, squares = exchange(sums, obs_weight, attitude_partials)
    results = settle(
        tile_pixel, pixel_slot, tile_knot[None, :], residual, obs_weight, source_partials,
        attitude_partials, source_index, table, squares, span,
    )
    return finish(*results)


def solution(mesh):
    in_specs = (
        P(("tm", "sky"), None),
        P(("tm", "sky"), None),
        P(None, ("tm", "sky"), None),
        P(None, ("tm", "sky"), None),
        P(("tm", "sky"), None),
        P(("tm", "sky")),
        P(("tm", "sky")),
        P(),
    )
    out_specs = (P(("tm", "sky"), None), P(None, "sky"), P(None, "tm"))
    return jax.shard_map(body, mesh=mesh, in_specs=in_specs, out_specs=out_specs, check_vma=False)
```

```python
import functools

import jax
import jax.numpy as jnp
from jax import lax
from jax.experimental import pallas as pl
from jax.experimental.pallas import tpu as pltpu
from jax.sharding import PartitionSpec as P

KNOTS_DEV = 512
ROWS = 20
PAD = 24
UPD = 5
LANES = 128
SUB = 8
MIB = 1024 * 1024

SOURCE_PAIRS = tuple(((first, second) for first in range(5) for second in range(first, 5)))
KNOT_PAIRS = tuple(((first, second) for first in range(4) for second in range(first, 4)))


def damped_solve(normal, target, order, pairs):
    entries = {}
    for number, couple in enumerate(pairs):
        entries[couple] = normal[number]
    factor, inverse = {}, []
    for column in range(order):
        pivot_value = entries[column, column] + 1.0
        for earlier in range(column):
            pivot_value = pivot_value - factor[column, earlier] * factor[column, earlier]
        inverse.append(1.0 / jnp.sqrt(pivot_value))
        for below in range(column + 1, order):
            current = entries[column, below]
            for earlier in range(column):
                current = current - factor[below, earlier] * factor[column, earlier]
            factor[below, column] = current * inverse[column]
    forward = []
    for column in range(order):
        current = target[column]
        for earlier in range(column):
            current = current - factor[column, earlier] * forward[earlier]
        forward.append(current * inverse[column])
    answer = [None] * order
    for column in reversed(range(order)):
        current = forward[column]
        for later in range(column + 1, order):
            current = current - factor[later, column] * answer[later]
        answer[column] = current * inverse[column]
    return answer


def split_times(times):
    inner = 2 if times % 2 == 0 else 1
    return times // inner, inner


def sums_kernel(
    tiles_step, pixel_hbm, slot_hbm, resid_hbm, weight_hbm, parts_hbm, index_hbm, out,
    pixel_ref, slot_ref, resid, weight, parts, index, stage, prods, sems,
):
    copies = [
        pltpu.make_async_copy(source, target, sems.at[number])
        for number, (source, target) in enumerate(
            [
                (pixel_hbm, pixel_ref),
                (slot_hbm, slot_ref),
                (resid_hbm, resid),
                (weight_hbm, weight),
                (parts_hbm, parts),
                (index_hbm, index),
            ]
        )
    ]
    for copy in copies:
        copy.start()
    tiles = resid.shape[0]
    zero = jnp.zeros((256, LANES), jnp.float32)

    def clear(step, carry):
        out[pl.ds(pl.multiple_of(step * 256, 256), 256), :] = zero
        return carry

    lax.fori_loop(0, out.shape[0] // 256, clear, 0)
    stage[...] = jnp.zeros_like(stage)
    sources = lax.broadcasted_iota(jnp.int32, (SUB, LANES), 0).astype(jnp.float32)
    bands = [
        jnp.concatenate([sources + float(16 * band), sources + float(16 * band + 8)], axis=0).astype(jnp.bfloat16)
        for band in range(LANES // 16)
    ]
    lanes_of = jnp.concatenate(bands, axis=0)
    one = jnp.ones((LANES, LANES), jnp.bfloat16)
    none = jnp.zeros((LANES, LANES), jnp.bfloat16)
    blank = jnp.zeros((2 * PAD, LANES), jnp.bfloat16)
    for copy in copies:
        copy.wait()

    def accumulate(step, slot):
        for j in range(tiles_step):
            start = slot_ref[pixel_ref[step * tiles_step + j]] * ROWS
            values = prods[pl.ds(slot * tiles_step * PAD + j * PAD, PAD), :]
            out[pl.ds(start, ROWS), :] += values[:ROWS]

    def multiply(step, slot):
        for part in range(tiles_step // SUB):
            base = pl.multiple_of(step * tiles_step + part * SUB, SUB)
            here = pl.ds(base, SUB)
            fields = [parts[c, here, :] for c in range(5)]
            scaled = [weight[here, :] * field for field in fields]
            baseline = resid[here, :]
            row = part * SUB * PAD
            for first, second in SOURCE_PAIRS:
                stage[pl.ds(row, SUB, stride=PAD), :] = scaled[first] * fields[second]
                row += 1
            for first in range(5):
                stage[pl.ds(row, SUB, stride=PAD), :] = scaled[first] * baseline
                row += 1
            ids = index[here, :].astype(jnp.float32)
            for j in range(0, SUB, 2):
                row = (part * SUB + j) * PAD
                lhs, hits = [], []
                for side in range(2):
                    values = stage[row + side * PAD : row + (side + 1) * PAD, :]
                    high = values.astype(jnp.bfloat16).astype(jnp.float32)
                    both = jnp.concatenate([high, values - high], axis=0).astype(jnp.bfloat16)
                    lhs.append(jnp.concatenate([both, blank] if side == 0 else [blank, both], axis=1))
                    wide = jnp.broadcast_to(ids[j + side : j + side + 1, :], (16, LANES)).astype(jnp.bfloat16)
                    tall = jnp.concatenate([wide] * (LANES // 16), axis=0)
                    hits.append(jnp.where(lanes_of == tall, one, none))
                got = lax.dot_general(
                    jnp.concatenate(lhs, axis=0),
                    jnp.concatenate(hits, axis=1),
                    (((1,), (1,)), ((), ())),
                    preferred_element_type=jnp.float32,
                )
                for side in range(2):
                    low = 2 * side * PAD
                    prods[pl.ds(slot * tiles_step * PAD + row + side * PAD, PAD), :] = (
                        got[low : low + PAD] + got[low + PAD : low + 2 * PAD]
                    )

    steps = tiles // tiles_step
    multiply(0, 0)

    def pair(step, carry):
        multiply(2 * step + 1, 1)
        accumulate(2 * step, 0)
        multiply(jnp.minimum(2 * step + 2, steps - 1), 0)
        accumulate(2 * step + 1, 1)
        return carry

    lax.fori_loop(0, steps // 2, pair, 0)


def local_sums(tile_pixel, pixel_slot, residual, obs_weight, source_partials, source_index):
    pixels = pixel_slot.shape[0]
    tiles_step = 32
    return pl.pallas_call(
        functools.partial(sums_kernel, tiles_step),
        name="local_sums",
        out_shape=jax.ShapeDtypeStruct((pixels * ROWS, LANES), jnp.float32),
        in_specs=[pl.BlockSpec(memory_space=pltpu.HBM)] * 6,
        out_specs=pl.BlockSpec(memory_space=pltpu.VMEM),
        scratch_shapes=[
            pltpu.SMEM(tile_pixel.shape, jnp.int32),
            pltpu.SMEM(pixel_slot.shape, jnp.int32),
            pltpu.VMEM(residual.shape, jnp.float32),
            pltpu.VMEM(obs_weight.shape, jnp.float32),
            pltpu.VMEM(source_partials.shape, jnp.float32),
            pltpu.VMEM(source_index.shape, jnp.int32),
            pltpu.VMEM((tiles_step * PAD, LANES), jnp.float32),
            pltpu.VMEM((2 * tiles_step * PAD, LANES), jnp.float32),
            pltpu.SemaphoreType.DMA((6,)),
        ],
        compiler_params=pltpu.CompilerParams(vmem_limit_bytes=18 * MIB),
    )(*[pltpu.with_memory_space_constraint(v, pltpu.HBM) for v in (tile_pixel, pixel_slot, residual, obs_weight, source_partials, source_index)])


def add_rows(target, *sources):
    rows = target.shape[0]
    step_rows = next(size for size in range(160, 0, -SUB) if rows % size == 0)

    def one(step, carry):
        here = pl.ds(pl.multiple_of(step * step_rows, step_rows), step_rows)
        total = sources[0][here, :]
        for source in sources[1:]:
            total = total + source[here, :]
        target[here, :] = total
        return carry

    lax.fori_loop(0, rows // step_rows, one, 0)


def square_sums(weight, att, rows, first, last):
    lane = lax.broadcasted_iota(jnp.int32, (SUB, LANES), 1)

    def group(step, carry):
        for part in range(2):
            here = pl.ds(pl.multiple_of(step * 2 * SUB + part * SUB, SUB), SUB)
            scale = weight[here, :]
            total = jnp.zeros((SUB, LANES), jnp.float32)
            for m in range(4):
                fields = [att[4 * m + c, here, :] for c in range(4)]
                scaled = [scale * field for field in fields]
                for number, (a, b) in enumerate(KNOT_PAIRS):
                    value = jnp.sum(scaled[a] * fields[b], axis=1, keepdims=True)
                    total = jnp.where(lane == 16 * m + number, value, total)
            rows[here, :] = total
        return carry

    lax.fori_loop(first, last, group, 0)


def exchange_kernel(
    times, lines, subs, units, depth, far_rows, sums, weight, att, table, squares,
    got0, gotz, gz2, a1, b1, a2, b2, part, got2, mine, upd, *sems
):
    (
        s0, r0, sz, rz, sy, ry, sa1, ra1, sb1, rb1, sa2, ra2, sb2, rb2, s3, r3, su, ru, st, rt, sd, rd,
    ) = sems
    outer, inner = split_times(times)
    mesh_ids = pl.DeviceIdType.MESH
    time, sky = lax.axis_index("tm"), lax.axis_index("sky")
    line, core = sky // 2, sky % 2
    mo, mi = time // inner, time % inner
    partner = (time, sky + 1 - 2 * core)
    tiles = weight.shape[0]
    rows = got0.shape[2]
    inner_at = [lax.rem(mi + step, inner) for step in range(1, inner)]
    outer_at = [lax.rem(mo + step, outer) for step in range(1, outer)]
    inner_peers = [(mo * inner + i, sky) for i in inner_at]
    outer_peers = [(o * inner + mi, sky) for o in outer_at]
    odd = [mask for mask in range(lines - 1, 1, -1) if mask % 2]
    even = [mask for mask in range(lines - 1, 0, -1) if mask % 2 == 0]
    masks = odd + even + ([1] if lines > 1 else [])
    direct = [mask for mask in masks if mask not in odd]
    line_of = {mask: jnp.bitwise_xor(line, mask) for mask in range(lines)}
    line_peer = {mask: (time, line_of[mask] * 2 + core) for mask in direct}

    barrier = pltpu.get_barrier_semaphore()
    peers = [partner] + inner_peers + outer_peers + [line_peer[mask] for mask in direct]
    for peer in peers:
        pl.semaphore_signal(barrier, inc=1, device_id=peer, device_id_type=mesh_ids)
    pl.semaphore_wait(barrier, len(peers))

    pending = []

    def send(source, target, send_sem, recv_sem, peer):
        copy = pltpu.make_async_remote_copy(
            src_ref=source, dst_ref=target, send_sem=send_sem, recv_sem=recv_sem,
            device_id=peer, device_id_type=mesh_ids,
        )
        copy.start()
        pending.append(copy)
        return copy

    pieces = [(mask, sub) for mask in masks + [0] for sub in range(subs)]
    count = len(pieces)
    zeroth, far_zeroth, far_third = {}, {}, {}
    far_at = pl.ds(subs * rows, far_rows)

    def stage_zero(k):
        mask, sub = pieces[k]
        zeroth[k] = send(
            sums.at[line_of[mask], 1 - core, :, pl.ds(sub * rows, rows)], got0.at[k], s0.at[k], r0.at[k], partner
        )

    def far_zero(mask):
        far_zeroth[mask] = send(
            sums.at[line_of[mask], 1 - core, :, far_at], gotz.at[mask], sz.at[mask], rz.at[mask], partner
        )

    far_order = masks + [0]
    for k in range(max(count, lines)):
        if k < count:
            stage_zero(k)
        if k < lines:
            far_zero(far_order[k])

    def far_add(mask):
        far_zeroth[mask].wait_recv()
        for t in range(times):
            add_rows(gotz.at[mask, t], gotz.at[mask, t], sums.at[line_of[mask], core, t, far_at])

    def far_send(mask):
        if mask in even and mask + 1 < lines:
            far_third[mask + 1].wait_recv()
            for t in range(times):
                add_rows(gotz.at[mask, t], gotz.at[mask, t], gz2.at[mask + 1, t])
        peer = line_peer[mask if mask in direct else 1]
        far_third[mask] = send(gotz.at[mask], gz2.at[mask], sy.at[mask], ry.at[mask], peer)

    def far_close():
        for mask in direct:
            far_third[mask].wait_recv()
        for t in range(times):
            add_rows(gotz.at[0, t], gotz.at[0, t], *[gz2.at[mask, t] for mask in direct])

    first_a, first_b, second_a, second_b, third = {}, {}, {}, {}, {}

    def held(k):
        return (got0.at[k], rows // 2) if k < count else (gotz.at[0], far_rows // 2)

    def spot_a(k, o, i):
        ref, quarter = held(k)
        return ref.at[o * inner + i, pl.ds(0, quarter)]

    def spot_b(k, o, i):
        ref, quarter = held(k)
        return ref.at[o * inner + i, pl.ds(quarter, quarter)]

    def stage_one(k):
        quarter = held(k)[1]
        size = pl.ds(0, quarter)
        if k < count:
            mask, sub = pieces[k]
            zeroth[k].wait_recv()
        else:
            far_close()
        first_a[k], first_b[k] = [], []
        for at_o, o in enumerate(outer_at + [mo]):
            for at_i, i in enumerate(inner_at + [mi]):
                t = o * inner + i
                if k < count:
                    add_rows(
                        got0.at[k, t], got0.at[k, t],
                        sums.at[line_of[mask], core, t, pl.ds(sub * rows, rows)],
                    )
                if at_i < inner - 1:
                    first_a[k].append(
                        send(
                            spot_a(k, o, i), a1.at[k, at_i, o, size], sa1.at[k, at_i, at_o],
                            ra1.at[k, at_i, at_o], inner_peers[at_i],
                        )
                    )
                if at_o < outer - 1:
                    first_b[k].append(
                        send(
                            spot_b(k, o, i), b1.at[k, at_o, i, size], sb1.at[k, at_o, at_i],
                            rb1.at[k, at_o, at_i], outer_peers[at_o],
                        )
                    )

    def stage_two(k):
        size = pl.ds(0, held(k)[1])
        for copy in first_a[k]:
            copy.wait_recv()
        second_a[k] = []
        for at_o, o in enumerate(outer_at + [mo]):
            own = spot_a(k, o, mi)
            add_rows(own, own, *[a1.at[k, number, o, size] for number in range(inner - 1)])
            if at_o < outer - 1:
                second_a[k].append(
                    send(own, a2.at[k, at_o, size], sa2.at[k, at_o], ra2.at[k, at_o], outer_peers[at_o])
                )
        for copy in first_b[k]:
            copy.wait_recv()
        second_b[k] = []
        for at_i, i in enumerate(inner_at + [mi]):
            own = spot_b(k, mo, i)
            add_rows(own, own, *[b1.at[k, number, i, size] for number in range(outer - 1)])
            if at_i < inner - 1:
                second_b[k].append(
                    send(own, b2.at[k, at_i, size], sb2.at[k, at_i], rb2.at[k, at_i], inner_peers[at_i])
                )

    def stage_three(k):
        quarter = held(k)[1]
        size = pl.ds(0, quarter)
        if k >= count:
            mask, sub, target, base = 0, subs, mine, subs * rows
        elif pieces[k][0]:
            (mask, sub), target, base = pieces[k], part.at[k], 0
        else:
            (mask, sub), target, base = pieces[k], mine, pieces[k][1] * rows
        extra = []
        if mask in even and mask + 1 < lines:
            third[mask + 1, sub].wait_recv()
            extra = [got2.at[pieces.index((mask + 1, sub))]]
        elif mask == 0 and k < count:
            for other in direct:
                third[other, sub].wait_recv()
            extra = [got2.at[pieces.index((other, sub))] for other in direct]
        for copy in second_a[k]:
            copy.wait_recv()
        add_rows(
            target.at[pl.ds(base, quarter)], spot_a(k, mo, mi),
            *[a2.at[k, number, size] for number in range(outer - 1)],
            *[ref.at[size] for ref in extra],
        )
        for copy in second_b[k]:
            copy.wait_recv()
        add_rows(
            target.at[pl.ds(base + quarter, quarter)], spot_b(k, mo, mi),
            *[b2.at[k, number, size] for number in range(inner - 1)],
            *[ref.at[pl.ds(quarter, quarter)] for ref in extra],
        )
        if mask:
            peer = line_peer[mask if mask in direct else 1]
            third[mask, sub] = send(part.at[k], got2.at[k], s3.at[k], r3.at[k], peer)

    groups = tiles // (2 * SUB)
    shares = 4
    total = count + 1
    for at in range(depth):
        stage_one(at)
        far_add(far_order[at])
        if far_order[at] in odd or far_order[at] == 1:
            far_send(far_order[at])
    waiting = [mask for mask in far_order[depth:]]
    late = [mask for mask in far_order[:depth] if mask in even]
    for k in range(total):
        if k < shares:
            square_sums(weight, att, squares, groups * k // shares, groups * (k + 1) // shares)
        stage_two(k)
        if k + depth < total:
            stage_one(k + depth)
        if waiting and k < depth:
            for mask in waiting:
                far_add(mask)
                if mask in odd or mask == 1:
                    far_send(mask)
                elif mask in even:
                    late.append(mask)
            waiting = []
        elif late:
            for mask in late:
                far_send(mask)
            late = []
        if k > 0:
            stage_three(k - 1)
    stage_three(total - 1)

    run = mine.shape[0] // ROWS
    block = run * UPD
    unit = block // units
    half_unit = unit // 2

    def spot(mask, source_time, sub):
        base = ((line_of[mask] * 2 + core) * times + source_time) * block + sub * unit
        return pl.multiple_of(base, SUB)

    from_line, near, far = {}, {}, {}

    def spread(mask, sub):
        place = table.at[pl.ds(spot(mask, time, sub), unit)]
        held_in = place
        if mask:
            from_line[mask, sub].wait_recv()
            if mask in even and mask + 1 < lines:
                from_line[mask + 1, sub] = send(
                    place, place, su.at[mask + 1, sub], ru.at[mask + 1, sub], line_peer[1]
                )
        else:
            held_in = upd.at[pl.ds(sub * unit, unit)]
        near[mask, sub] = [
            send(held_in, place, st.at[mask, sub, number], rt.at[mask, sub, number], peer)
            for number, peer in enumerate(inner_peers + outer_peers)
        ]

    def relay(mask, sub):
        far[mask, sub] = []
        number = inner + outer - 2
        for which, copy in enumerate(near[mask, sub]):
            copy.wait_recv()
            if which < inner - 1:
                origin = mo * inner + lax.rem(mi + inner - (which + 1), inner)
                start, targets = 0, outer_peers
            else:
                origin = lax.rem(mo + outer - (which - inner + 2), outer) * inner + mi
                start, targets = half_unit, inner_peers
            piece = table.at[pl.ds(pl.multiple_of(spot(mask, origin, sub) + start, SUB), half_unit)]
            for peer in targets:
                far[mask, sub].append(
                    send(piece, piece, st.at[mask, sub, number], rt.at[mask, sub, number], peer)
                )
                number += 1

    def conclude(mask):
        for sub in range(units):
            for copy in far[mask, sub]:
                copy.wait_recv()
        place = table.at[pl.ds(spot(mask, 0, 0), times * block)]
        return send(place, place, sd.at[mask], rd.at[mask], partner)

    for sub in range(units):
        pixels = run // units

        starts = [sub * pixels + start for start in range(0, pixels, SUB)]
        entry = [
            jnp.concatenate([mine[pl.ds(start * ROWS + row, SUB, stride=ROWS), :] for start in starts], axis=0)
            for row in range(ROWS)
        ]
        answer = damped_solve(entry[:15], entry[15:], 5, SOURCE_PAIRS)
        for c in range(UPD):
            for number, start in enumerate(starts):
                upd[pl.ds(start * UPD + c, SUB, stride=UPD), :] = answer[c][number * SUB : (number + 1) * SUB]
        for mask in even + [1]:
            from_line[mask, sub] = send(
                upd.at[pl.ds(sub * unit, unit)], table.at[pl.ds(spot(0, time, sub), unit)],
                su.at[mask, sub], ru.at[mask, sub], line_peer[mask],
            )
        spread(0, sub)
        table[pl.ds(spot(0, time, sub), unit), :] = upd[sub * unit : (sub + 1) * unit, :]

    ordered = [0, 1] + even[::-1] + odd[::-1]
    def each(step, *group):
        for mask in group:
            for sub in range(units):
                step(mask, sub)

    each(spread, 1, *even[::-1])
    each(relay, 0, 1)
    each(spread, *odd[::-1])
    each(relay, *even[::-1])
    last = [conclude(0)]
    each(relay, *odd[::-1])
    last += [conclude(mask) for mask in ordered[1:]]
    for copy in last:
        copy.wait_recv()
    for copy in pending:
        copy.wait_send()


def exchange(sums, obs_weight, attitude_partials):
    times, owners = lax.axis_size("tm"), lax.axis_size("sky")
    lines = owners // 2
    outer, inner = split_times(times)
    total_rows = sums.shape[0]
    chunk = total_rows // (owners * times)
    pixels = total_rows // ROWS
    block = chunk // ROWS * UPD
    far_rows = chunk // 4
    rest = chunk - far_rows
    subs = 2 if rest % 32 == 0 else 1
    units = 2 if block % 32 == 0 else 1
    rows = rest // subs
    quarter = max(rows, far_rows) // 2
    tiles = obs_weight.shape[0]
    count = lines * subs
    total = count + 1
    dma = pltpu.SemaphoreType.DMA
    vmem = pltpu.VMEM
    near = inner + outer - 2
    far = 2 * (inner - 1) * (outer - 1)
    f32 = jnp.float32

    def pair(*shape):
        return [dma(shape), dma(shape)]

    return pl.pallas_call(
        functools.partial(exchange_kernel, times, lines, subs, units, 2, far_rows),
        name="exchange",
        out_shape=(
            jax.ShapeDtypeStruct((pixels * UPD + SUB, LANES), f32),
            jax.ShapeDtypeStruct((tiles, LANES), f32),
        ),
        in_specs=[pl.BlockSpec(memory_space=pltpu.VMEM)] * 3,
        out_specs=(pl.BlockSpec(memory_space=pltpu.VMEM),) * 2,
        scratch_shapes=[
            vmem((count, times, rows, LANES), f32),
            vmem((lines, times, far_rows, LANES), f32),
            vmem((lines, times, far_rows, LANES), f32),
            vmem((total, max(inner - 1, 1), outer, quarter, LANES), f32),
            vmem((total, max(outer - 1, 1), inner, quarter, LANES), f32),
            vmem((total, max(outer - 1, 1), quarter, LANES), f32),
            vmem((total, max(inner - 1, 1), quarter, LANES), f32),
            vmem((count, rows, LANES), f32),
            vmem((count, rows, LANES), f32),
            vmem((chunk, LANES), f32),
            vmem((block, LANES), f32),
        ]
        + pair(count)
        + pair(lines)
        + pair(lines)
        + pair(total, max(inner - 1, 1), outer)
        + pair(total, max(outer - 1, 1), inner)
        + pair(total, max(outer - 1, 1))
        + pair(total, max(inner - 1, 1))
        + pair(count)
        + pair(lines, units)
        + pair(lines, units, near + far)
        + pair(lines),
        compiler_params=pltpu.CompilerParams(
            collective_id=0, has_side_effects=True, vmem_limit_bytes=24 * MIB
        ),
    )(sums.reshape(lines, 2, times, chunk, LANES), obs_weight, attitude_partials)


def thirds(value):
    high = value.astype(jnp.bfloat16)
    rest = value - high.astype(jnp.float32)
    middle = rest.astype(jnp.bfloat16)
    return high, middle, (rest - middle.astype(jnp.float32)).astype(jnp.bfloat16)


def settle_kernel(
    times, owners, span, pixel_hbm, slot_hbm, knots, resid, weight, parts, att, index, table, squares,
    out, source_out, knot_out, pixel_ref, slot_ref, rows, terms, sums, before, mine, after, settles, values, others,
    sp, sl, sa, ra, sb, rb, sc, rc,
):
    mesh_ids = pl.DeviceIdType.MESH
    time, sky = lax.axis_index("tm"), lax.axis_index("sky")
    blocks = times * owners
    block = time * owners + sky
    nxt, prev = lax.rem(block + 1, blocks), lax.rem(block + blocks - 1, blocks)
    next_id, prev_id = (nxt // owners, lax.rem(nxt, owners)), (prev // owners, lax.rem(prev, owners))
    peers = [(time, lax.rem(sky + step, owners)) for step in range(1, owners)]
    barrier = pltpu.get_barrier_semaphore()
    for peer in [next_id, prev_id] + peers:
        pl.semaphore_signal(barrier, inc=1, device_id=peer, device_id_type=mesh_ids)

    pixels_in = pltpu.make_async_copy(pixel_hbm, pixel_ref, sp)
    slots_in = pltpu.make_async_copy(slot_hbm, slot_ref, sl)
    pixels_in.start()
    slots_in.start()
    pixels_in.wait()
    slots_in.wait()
    tiles = resid.shape[0]
    lane = lax.broadcasted_iota(jnp.int32, (SUB, LANES), 1)
    unroll = rows.shape[0]

    def group(step, carry):
        for part in range(unroll):
            base = pl.multiple_of((step * unroll + part) * SUB, SUB)
            here = pl.ds(base, SUB)
            for j in range(SUB):
                seat = slot_ref[pixel_ref[base + j]]
                rows[part, j * SUB : (j + 1) * SUB, :] = table[pl.ds(seat * UPD, SUB), :]
            ids = index[here, :]
            total = None
            for c in range(UPD):
                picked = jnp.take_along_axis(rows[part, pl.ds(c, SUB, stride=SUB), :], ids, axis=1)
                addend = parts[c, here, :] * picked
                total = addend if total is None else total + addend
            settled = resid[here, :] - total
            settles[here, :] = settled
            scaled = weight[here, :] * settled
            term = squares[here, :]
            for m in range(4):
                for c in range(4):
                    value = jnp.sum(scaled * att[4 * m + c, here, :], axis=1, keepdims=True)
                    term = jnp.where(lane == 16 * m + 10 + c, value, term)
            terms[here, :] = term
        return carry

    lax.fori_loop(0, tiles // (SUB * unroll), group, 0)
    knot = lax.broadcasted_iota(jnp.int32, (LANES, tiles), 0) + block * span
    hits = jnp.where(knot == knots[...], 1.0, 0.0).astype(jnp.bfloat16)
    placed = None
    for piece in thirds(terms[...]):
        got = jnp.dot(hits, piece, preferred_element_type=jnp.float32)
        placed = got if placed is None else placed + got
    turned = placed.T
    total = turned[:16]
    for m in range(1, 4):
        total = total + pltpu.roll(turned[16 * m : 16 * m + 16], m, 1)
    sums[...] = total

    pl.semaphore_wait(barrier, owners + 1)
    pending = []

    def send(source, target, send_sem, recv_sem, peer):
        copy = pltpu.make_async_remote_copy(
            src_ref=source, dst_ref=target, send_sem=send_sem, recv_sem=recv_sem,
            device_id=peer, device_id_type=mesh_ids,
        )
        copy.start()
        pending.append(copy)
        return copy

    handed = [send(sums, before, sa, ra, next_id), send(sums, after, sb, rb, prev_id)]
    per_owner = source_out.shape[1] // LANES

    def spread(step, carry):
        for part in range(SUB):
            pixel = step * SUB + part
            place = pl.ds(pl.multiple_of(pixel * LANES, LANES), LANES)
            source_out[:, place] = table[pl.ds((sky * per_owner + pixel) * UPD, UPD), :]
        return carry

    lax.fori_loop(0, per_owner // SUB, spread, 0)
    wide = lax.broadcasted_iota(jnp.int32, (16, LANES), 1)
    for copy in handed:
        copy.wait_recv()
    head = pltpu.roll(before[...], LANES - span, 1)
    tail = pltpu.roll(after[...], span, 1)
    whole = sums[...] + jnp.where((wide < 3) & (block > 0), head, 0.0)
    whole = whole + jnp.where((wide >= span) & (wide < span + 3), tail, 0.0)
    answer = damped_solve(
        [whole[n : n + 1] for n in range(10)], [whole[n : n + 1] for n in range(10, 14)], 4, KNOT_PAIRS
    )
    for c in range(4):
        mine[c : c + 1, :] = answer[c]
        mine[4 + c : 5 + c, :] = answer[c]
    around = [
        send(mine, others.at[sky], sc.at[number], rc.at[number], peer)
        for number, peer in enumerate(peers)
    ]
    others[pl.ds(sky, 1)] = mine[...][None]
    reach = jnp.where(block < blocks - 1, span + 3, span)
    extended = jnp.where(lane < reach, mine[...], 0.0)
    windows = []
    for m in range(0, 4, 2):
        low = extended if m == 0 else pltpu.roll(extended, LANES - m, 1)
        high = pltpu.roll(extended, LANES - m - 1, 1)
        half = lax.broadcasted_iota(jnp.int32, (SUB, LANES), 0) < 4
        windows.append(jnp.where(half, low, high))
    window = jnp.concatenate(windows, axis=0)
    picked = None
    for piece in thirds(window):
        got = jnp.dot(piece, hits, preferred_element_type=jnp.float32)
        picked = got if picked is None else picked + got
    for part in range(tiles // LANES):
        values[part * LANES : (part + 1) * LANES, :] = picked[:, part * LANES : (part + 1) * LANES].T

    def last(step, carry):
        for part in range(unroll):
            here = pl.ds(pl.multiple_of((step * unroll + part) * SUB, SUB), SUB)
            column = values[here, :]
            total = None
            for number in range(16):
                addend = att[number, here, :] * column[:, number : number + 1]
                total = addend if total is None else total + addend
            out[here, :] = settles[here, :] - total
        return carry

    lax.fori_loop(0, tiles // (SUB * unroll), last, 0)
    for copy in around:
        copy.wait_recv()
    each = LANES // span
    for first in range(0, owners, each):
        joined = jnp.where(lane < span, others[first], 0.0)
        for number in range(1, each):
            moved = pltpu.roll(others[first + number], number * span, 1)
            keep = (lane >= number * span) & (lane < (number + 1) * span)
            joined = jnp.where(keep, moved, joined)
        knot_out[:, first * span : first * span + LANES] = joined[:4]
    for copy in pending:
        copy.wait_send()


def settle(tile_pixel, pixel_slot, knots, residual, obs_weight, source_partials, attitude_partials, source_index, table, squares, span):
    times, owners = lax.axis_size("tm"), lax.axis_size("sky")
    tiles = residual.shape[0]
    unroll = 8
    pixels = pixel_slot.shape[0]
    dma = pltpu.SemaphoreType.DMA
    f32 = jnp.float32
    return pl.pallas_call(
        functools.partial(settle_kernel, times, owners, span),
        name="settle",
        out_shape=(
            jax.ShapeDtypeStruct(residual.shape, f32),
            jax.ShapeDtypeStruct((UPD, pixels // owners * LANES), f32),
            jax.ShapeDtypeStruct((4, span * owners), f32),
        ),
        in_specs=[pl.BlockSpec(memory_space=pltpu.HBM)] * 2 + [pl.BlockSpec(memory_space=pltpu.VMEM)] * 8,
        out_specs=(pl.BlockSpec(memory_space=pltpu.VMEM),) * 3,
        scratch_shapes=[
            pltpu.SMEM(tile_pixel.shape, jnp.int32),
            pltpu.SMEM(pixel_slot.shape, jnp.int32),
            pltpu.VMEM((unroll, SUB * SUB, LANES), f32),
            pltpu.VMEM((tiles, LANES), f32),
            pltpu.VMEM((16, LANES), f32),
            pltpu.VMEM((16, LANES), f32),
            pltpu.VMEM((SUB, LANES), f32),
            pltpu.VMEM((16, LANES), f32),
            pltpu.VMEM(residual.shape, f32),
            pltpu.VMEM((tiles, 16), f32),
            pltpu.VMEM((owners, SUB, LANES), f32),
            dma, dma, dma, dma, dma, dma, dma((owners - 1,)), dma((owners - 1,)),
        ],
        compiler_params=pltpu.CompilerParams(
            collective_id=1, has_side_effects=True, vmem_limit_bytes=24 * MIB
        ),
    )(tile_pixel, pixel_slot, knots, residual, obs_weight, source_partials, attitude_partials, source_index, table, squares)


def finish_kernel(*refs):
    count = (len(refs) - 1) // 2
    copies = [
        pltpu.make_async_copy(refs[number], refs[count + number], refs[-1].at[number]) for number in range(count)
    ]
    for copy in copies:
        copy.start()
    for copy in copies:
        copy.wait()


def finish(*results):
    return pl.pallas_call(
        finish_kernel,
        name="finish",
        out_shape=tuple(jax.ShapeDtypeStruct(value.shape, value.dtype) for value in results),
        in_specs=[pl.BlockSpec(memory_space=pltpu.VMEM)] * len(results),
        out_specs=(pl.BlockSpec(memory_space=pltpu.HBM),) * len(results),
        scratch_shapes=[pltpu.SemaphoreType.DMA((len(results),))],
        compiler_params=pltpu.CompilerParams(vmem_limit_bytes=8 * MIB),
    )(*results)


def body(residual, obs_weight, source_partials, attitude_partials, source_index, tile_pixel, tile_knot, pixel_slot):
    span = KNOTS_DEV // lax.axis_size("sky")
    sums = local_sums(tile_pixel, pixel_slot, residual, obs_weight, source_partials, source_index)
    table, squares = exchange(sums, obs_weight, attitude_partials)
    results = settle(
        tile_pixel, pixel_slot, tile_knot[None, :], residual, obs_weight, source_partials,
        attitude_partials, source_index, table, squares, span,
    )
    return finish(*results)


def solution(mesh):
    in_specs = (
        P(("tm", "sky"), None),
        P(("tm", "sky"), None),
        P(None, ("tm", "sky"), None),
        P(None, ("tm", "sky"), None),
        P(("tm", "sky"), None),
        P(("tm", "sky")),
        P(("tm", "sky")),
        P(),
    )
    out_specs = (P(("tm", "sky"), None), P(None, "sky"), P(None, "tm"))
    return jax.shard_map(body, mesh=mesh, in_specs=in_specs, out_specs=out_specs, check_vma=False)
```

```python
import functools

import jax
import jax.numpy as jnp
from jax import lax
from jax.experimental import pallas as pl
from jax.experimental.pallas import tpu as pltpu
from jax.sharding import PartitionSpec as P

KNOTS_DEV = 512
ROWS = 20
PAD = 24
UPD = 5
LANES = 128
SUB = 8
MIB = 1024 * 1024

SOURCE_PAIRS = tuple(((first, second) for first in range(5) for second in range(first, 5)))
KNOT_PAIRS = tuple(((first, second) for first in range(4) for second in range(first, 4)))


def damped_solve(normal, target, order, pairs):
    entries = {}
    for number, couple in enumerate(pairs):
        entries[couple] = normal[number]
    factor, inverse = {}, []
    for column in range(order):
        pivot_value = entries[column, column] + 1.0
        for earlier in range(column):
            pivot_value = pivot_value - factor[column, earlier] * factor[column, earlier]
        inverse.append(1.0 / jnp.sqrt(pivot_value))
        for below in range(column + 1, order):
            current = entries[column, below]
            for earlier in range(column):
                current = current - factor[below, earlier] * factor[column, earlier]
            factor[below, column] = current * inverse[column]
    forward = []
    for column in range(order):
        current = target[column]
        for earlier in range(column):
            current = current - factor[column, earlier] * forward[earlier]
        forward.append(current * inverse[column])
    answer = [None] * order
    for column in reversed(range(order)):
        current = forward[column]
        for later in range(column + 1, order):
            current = current - factor[later, column] * answer[later]
        answer[column] = current * inverse[column]
    return answer


def split_times(times):
    inner = 2 if times % 2 == 0 else 1
    return times // inner, inner


def sums_kernel(
    tiles_step, pixel_hbm, slot_hbm, resid_hbm, weight_hbm, parts_hbm, index_hbm, out,
    pixel_ref, slot_ref, resid, weight, parts, index, stage, prods, sems,
):
    copies = [
        pltpu.make_async_copy(source, target, sems.at[number])
        for number, (source, target) in enumerate(
            [
                (pixel_hbm, pixel_ref),
                (slot_hbm, slot_ref),
                (resid_hbm, resid),
                (weight_hbm, weight),
                (parts_hbm, parts),
                (index_hbm, index),
            ]
        )
    ]
    for copy in copies:
        copy.start()
    tiles = resid.shape[0]
    zero = jnp.zeros((256, LANES), jnp.float32)

    def clear(step, carry):
        out[pl.ds(pl.multiple_of(step * 256, 256), 256), :] = zero
        return carry

    lax.fori_loop(0, out.shape[0] // 256, clear, 0)
    stage[...] = jnp.zeros_like(stage)
    sources = lax.broadcasted_iota(jnp.int32, (SUB, LANES), 0).astype(jnp.float32)
    bands = [
        jnp.concatenate([sources + float(16 * band), sources + float(16 * band + 8)], axis=0).astype(jnp.bfloat16)
        for band in range(LANES // 16)
    ]
    lanes_of = jnp.concatenate(bands, axis=0)
    one = jnp.ones((LANES, LANES), jnp.bfloat16)
    none = jnp.zeros((LANES, LANES), jnp.bfloat16)
    blank = jnp.zeros((2 * PAD, LANES), jnp.bfloat16)
    for copy in copies:
        copy.wait()

    def accumulate(step, slot):
        for j in range(tiles_step):
            start = slot_ref[pixel_ref[step * tiles_step + j]] * ROWS
            values = prods[pl.ds(slot * tiles_step * PAD + j * PAD, PAD), :]
            out[pl.ds(start, ROWS), :] += values[:ROWS]

    def multiply(step, slot):
        for part in range(tiles_step // SUB):
            base = pl.multiple_of(step * tiles_step + part * SUB, SUB)
            here = pl.ds(base, SUB)
            fields = [parts[c, here, :] for c in range(5)]
            scaled = [weight[here, :] * field for field in fields]
            baseline = resid[here, :]
            row = part * SUB * PAD
            for first, second in SOURCE_PAIRS:
                stage[pl.ds(row, SUB, stride=PAD), :] = scaled[first] * fields[second]
                row += 1
            for first in range(5):
                stage[pl.ds(row, SUB, stride=PAD), :] = scaled[first] * baseline
                row += 1
            ids = index[here, :].astype(jnp.float32)
            for j in range(0, SUB, 2):
                row = (part * SUB + j) * PAD
                lhs, hits = [], []
                for side in range(2):
                    values = stage[row + side * PAD : row + (side + 1) * PAD, :]
                    high = values.astype(jnp.bfloat16).astype(jnp.float32)
                    both = jnp.concatenate([high, values - high], axis=0).astype(jnp.bfloat16)
                    lhs.append(jnp.concatenate([both, blank] if side == 0 else [blank, both], axis=1))
                    wide = jnp.broadcast_to(ids[j + side : j + side + 1, :], (16, LANES)).astype(jnp.bfloat16)
                    tall = jnp.concatenate([wide] * (LANES // 16), axis=0)
                    hits.append(jnp.where(lanes_of == tall, one, none))
                got = lax.dot_general(
                    jnp.concatenate(lhs, axis=0),
                    jnp.concatenate(hits, axis=1),
                    (((1,), (1,)), ((), ())),
                    preferred_element_type=jnp.float32,
                )
                for side in range(2):
                    low = 2 * side * PAD
                    prods[pl.ds(slot * tiles_step * PAD + row + side * PAD, PAD), :] = (
                        got[low : low + PAD] + got[low + PAD : low + 2 * PAD]
                    )

    steps = tiles // tiles_step
    multiply(0, 0)

    def pair(step, carry):
        multiply(2 * step + 1, 1)
        accumulate(2 * step, 0)
        multiply(jnp.minimum(2 * step + 2, steps - 1), 0)
        accumulate(2 * step + 1, 1)
        return carry

    lax.fori_loop(0, steps // 2, pair, 0)


def local_sums(tile_pixel, pixel_slot, residual, obs_weight, source_partials, source_index):
    pixels = pixel_slot.shape[0]
    tiles_step = 64
    return pl.pallas_call(
        functools.partial(sums_kernel, tiles_step),
        name="local_sums",
        out_shape=jax.ShapeDtypeStruct((pixels * ROWS, LANES), jnp.float32),
        in_specs=[pl.BlockSpec(memory_space=pltpu.HBM)] * 6,
        out_specs=pl.BlockSpec(memory_space=pltpu.VMEM),
        scratch_shapes=[
            pltpu.SMEM(tile_pixel.shape, jnp.int32),
            pltpu.SMEM(pixel_slot.shape, jnp.int32),
            pltpu.VMEM(residual.shape, jnp.float32),
            pltpu.VMEM(obs_weight.shape, jnp.float32),
            pltpu.VMEM(source_partials.shape, jnp.float32),
            pltpu.VMEM(source_index.shape, jnp.int32),
            pltpu.VMEM((tiles_step * PAD, LANES), jnp.float32),
            pltpu.VMEM((2 * tiles_step * PAD, LANES), jnp.float32),
            pltpu.SemaphoreType.DMA((6,)),
        ],
        compiler_params=pltpu.CompilerParams(vmem_limit_bytes=18 * MIB),
    )(*[pltpu.with_memory_space_constraint(v, pltpu.HBM) for v in (tile_pixel, pixel_slot, residual, obs_weight, source_partials, source_index)])


def add_rows(target, *sources):
    rows = target.shape[0]
    step_rows = next(size for size in range(160, 0, -SUB) if rows % size == 0)

    def one(step, carry):
        here = pl.ds(pl.multiple_of(step * step_rows, step_rows), step_rows)
        total = sources[0][here, :]
        for source in sources[1:]:
            total = total + source[here, :]
        target[here, :] = total
        return carry

    lax.fori_loop(0, rows // step_rows, one, 0)


def square_sums(weight, att, rows, first, last):
    lane = lax.broadcasted_iota(jnp.int32, (SUB, LANES), 1)

    def group(step, carry):
        for part in range(2):
            here = pl.ds(pl.multiple_of(step * 2 * SUB + part * SUB, SUB), SUB)
            scale = weight[here, :]
            total = jnp.zeros((SUB, LANES), jnp.float32)
            for m in range(4):
                fields = [att[4 * m + c, here, :] for c in range(4)]
                scaled = [scale * field for field in fields]
                for number, (a, b) in enumerate(KNOT_PAIRS):
                    value = jnp.sum(scaled[a] * fields[b], axis=1, keepdims=True)
                    total = jnp.where(lane == 16 * m + number, value, total)
            rows[here, :] = total
        return carry

    lax.fori_loop(first, last, group, 0)


def exchange_kernel(
    times, lines, subs, units, depth, far_rows, sums, weight, att, table, squares,
    got0, gotz, gz2, a1, b1, a2, b2, part, got2, mine, upd, *sems
):
    (
        s0, r0, sz, rz, sy, ry, sa1, ra1, sb1, rb1, sa2, ra2, sb2, rb2, s3, r3, su, ru, st, rt, sd, rd,
    ) = sems
    outer, inner = split_times(times)
    mesh_ids = pl.DeviceIdType.MESH
    time, sky = lax.axis_index("tm"), lax.axis_index("sky")
    line, core = sky // 2, sky % 2
    mo, mi = time // inner, time % inner
    partner = (time, sky + 1 - 2 * core)
    tiles = weight.shape[0]
    rows = got0.shape[2]
    inner_at = [lax.rem(mi + step, inner) for step in range(1, inner)]
    outer_at = [lax.rem(mo + step, outer) for step in range(1, outer)]
    inner_peers = [(mo * inner + i, sky) for i in inner_at]
    outer_peers = [(o * inner + mi, sky) for o in outer_at]
    odd = [mask for mask in range(lines - 1, 1, -1) if mask % 2]
    even = [mask for mask in range(lines - 1, 0, -1) if mask % 2 == 0]
    masks = odd + even + ([1] if lines > 1 else [])
    direct = [mask for mask in masks if mask not in odd]
    line_of = {mask: jnp.bitwise_xor(line, mask) for mask in range(lines)}
    line_peer = {mask: (time, line_of[mask] * 2 + core) for mask in direct}

    barrier = pltpu.get_barrier_semaphore()
    peers = [partner] + inner_peers + outer_peers + [line_peer[mask] for mask in direct]
    for peer in peers:
        pl.semaphore_signal(barrier, inc=1, device_id=peer, device_id_type=mesh_ids)
    pl.semaphore_wait(barrier, len(peers))

    pending = []

    def send(source, target, send_sem, recv_sem, peer):
        copy = pltpu.make_async_remote_copy(
            src_ref=source, dst_ref=target, send_sem=send_sem, recv_sem=recv_sem,
            device_id=peer, device_id_type=mesh_ids,
        )
        copy.start()
        pending.append(copy)
        return copy

    pieces = [(mask, sub) for mask in masks + [0] for sub in range(subs)]
    count = len(pieces)
    zeroth, far_zeroth, far_third = {}, {}, {}
    far_at = pl.ds(subs * rows, far_rows)

    def stage_zero(k):
        mask, sub = pieces[k]
        zeroth[k] = send(
            sums.at[line_of[mask], 1 - core, :, pl.ds(sub * rows, rows)], got0.at[k], s0.at[k], r0.at[k], partner
        )

    def far_zero(mask):
        far_zeroth[mask] = send(
            sums.at[line_of[mask], 1 - core, :, far_at], gotz.at[mask], sz.at[mask], rz.at[mask], partner
        )

    far_order = masks + [0]
    for k in range(max(count, lines)):
        if k < count:
            stage_zero(k)
        if k < lines:
            far_zero(far_order[k])

    def far_add(mask):
        far_zeroth[mask].wait_recv()
        for t in range(times):
            add_rows(gotz.at[mask, t], gotz.at[mask, t], sums.at[line_of[mask], core, t, far_at])

    def far_send(mask):
        if mask in even and mask + 1 < lines:
            far_third[mask + 1].wait_recv()
            for t in range(times):
                add_rows(gotz.at[mask, t], gotz.at[mask, t], gz2.at[mask + 1, t])
        peer = line_peer[mask if mask in direct else 1]
        far_third[mask] = send(gotz.at[mask], gz2.at[mask], sy.at[mask], ry.at[mask], peer)

    def far_close():
        for mask in direct:
            far_third[mask].wait_recv()
        for t in range(times):
            add_rows(gotz.at[0, t], gotz.at[0, t], *[gz2.at[mask, t] for mask in direct])

    first_a, first_b, second_a, second_b, third = {}, {}, {}, {}, {}

    def held(k):
        return (got0.at[k], rows // 2) if k < count else (gotz.at[0], far_rows // 2)

    def spot_a(k, o, i):
        ref, quarter = held(k)
        return ref.at[o * inner + i, pl.ds(0, quarter)]

    def spot_b(k, o, i):
        ref, quarter = held(k)
        return ref.at[o * inner + i, pl.ds(quarter, quarter)]

    def stage_one(k):
        quarter = held(k)[1]
        size = pl.ds(0, quarter)
        if k < count:
            mask, sub = pieces[k]
            zeroth[k].wait_recv()
        else:
            far_close()
        first_a[k], first_b[k] = [], []
        for at_o, o in enumerate(outer_at + [mo]):
            for at_i, i in enumerate(inner_at + [mi]):
                t = o * inner + i
                if k < count:
                    add_rows(
                        got0.at[k, t], got0.at[k, t],
                        sums.at[line_of[mask], core, t, pl.ds(sub * rows, rows)],
                    )
                if at_i < inner - 1:
                    first_a[k].append(
                        send(
                            spot_a(k, o, i), a1.at[k, at_i, o, size], sa1.at[k, at_i, at_o],
                            ra1.at[k, at_i, at_o], inner_peers[at_i],
                        )
                    )
                if at_o < outer - 1:
                    first_b[k].append(
                        send(
                            spot_b(k, o, i), b1.at[k, at_o, i, size], sb1.at[k, at_o, at_i],
                            rb1.at[k, at_o, at_i], outer_peers[at_o],
                        )
                    )

    def stage_two(k):
        size = pl.ds(0, held(k)[1])
        for copy in first_a[k]:
            copy.wait_recv()
        second_a[k] = []
        for at_o, o in enumerate(outer_at + [mo]):
            own = spot_a(k, o, mi)
            add_rows(own, own, *[a1.at[k, number, o, size] for number in range(inner - 1)])
            if at_o < outer - 1:
                second_a[k].append(
                    send(own, a2.at[k, at_o, size], sa2.at[k, at_o], ra2.at[k, at_o], outer_peers[at_o])
                )
        for copy in first_b[k]:
            copy.wait_recv()
        second_b[k] = []
        for at_i, i in enumerate(inner_at + [mi]):
            own = spot_b(k, mo, i)
            add_rows(own, own, *[b1.at[k, number, i, size] for number in range(outer - 1)])
            if at_i < inner - 1:
                second_b[k].append(
                    send(own, b2.at[k, at_i, size], sb2.at[k, at_i], rb2.at[k, at_i], inner_peers[at_i])
                )

    def stage_three(k):
        quarter = held(k)[1]
        size = pl.ds(0, quarter)
        if k >= count:
            mask, sub, target, base = 0, subs, mine, subs * rows
        elif pieces[k][0]:
            (mask, sub), target, base = pieces[k], part.at[k], 0
        else:
            (mask, sub), target, base = pieces[k], mine, pieces[k][1] * rows
        extra = []
        if mask in even and mask + 1 < lines:
            third[mask + 1, sub].wait_recv()
            extra = [got2.at[pieces.index((mask + 1, sub))]]
        elif mask == 0 and k < count:
            for other in direct:
                third[other, sub].wait_recv()
            extra = [got2.at[pieces.index((other, sub))] for other in direct]
        for copy in second_a[k]:
            copy.wait_recv()
        add_rows(
            target.at[pl.ds(base, quarter)], spot_a(k, mo, mi),
            *[a2.at[k, number, size] for number in range(outer - 1)],
            *[ref.at[size] for ref in extra],
        )
        for copy in second_b[k]:
            copy.wait_recv()
        add_rows(
            target.at[pl.ds(base + quarter, quarter)], spot_b(k, mo, mi),
            *[b2.at[k, number, size] for number in range(inner - 1)],
            *[ref.at[pl.ds(quarter, quarter)] for ref in extra],
        )
        if mask:
            peer = line_peer[mask if mask in direct else 1]
            third[mask, sub] = send(part.at[k], got2.at[k], s3.at[k], r3.at[k], peer)

    groups = tiles // (2 * SUB)
    shares = 4
    total = count + 1
    for at in range(depth):
        stage_one(at)
        far_add(far_order[at])
        if far_order[at] in odd or far_order[at] == 1:
            far_send(far_order[at])
    waiting = [mask for mask in far_order[depth:]]
    late = [mask for mask in far_order[:depth] if mask in even]
    for k in range(total):
        if k < shares:
            square_sums(weight, att, squares, groups * k // shares, groups * (k + 1) // shares)
        stage_two(k)
        if k + depth < total:
            stage_one(k + depth)
        if waiting and k < depth:
            for mask in waiting:
                far_add(mask)
                if mask in odd or mask == 1:
                    far_send(mask)
                elif mask in even:
                    late.append(mask)
            waiting = []
        elif late:
            for mask in late:
                far_send(mask)
            late = []
        if k > 0:
            stage_three(k - 1)
    stage_three(total - 1)

    run = mine.shape[0] // ROWS
    block = run * UPD
    unit = block // units
    half_unit = unit // 2

    def spot(mask, source_time, sub):
        base = ((line_of[mask] * 2 + core) * times + source_time) * block + sub * unit
        return pl.multiple_of(base, SUB)

    from_line, near, far = {}, {}, {}

    def spread(mask, sub):
        place = table.at[pl.ds(spot(mask, time, sub), unit)]
        held_in = place
        if mask:
            from_line[mask, sub].wait_recv()
            if mask in even and mask + 1 < lines:
                from_line[mask + 1, sub] = send(
                    place, place, su.at[mask + 1, sub], ru.at[mask + 1, sub], line_peer[1]
                )
        else:
            held_in = upd.at[pl.ds(sub * unit, unit)]
        near[mask, sub] = [
            send(held_in, place, st.at[mask, sub, number], rt.at[mask, sub, number], peer)
            for number, peer in enumerate(inner_peers + outer_peers)
        ]

    def relay(mask, sub):
        far[mask, sub] = []
        number = inner + outer - 2
        for which, copy in enumerate(near[mask, sub]):
            copy.wait_recv()
            if which < inner - 1:
                origin = mo * inner + lax.rem(mi + inner - (which + 1), inner)
                start, targets = 0, outer_peers
            else:
                origin = lax.rem(mo + outer - (which - inner + 2), outer) * inner + mi
                start, targets = half_unit, inner_peers
            piece = table.at[pl.ds(pl.multiple_of(spot(mask, origin, sub) + start, SUB), half_unit)]
            for peer in targets:
                far[mask, sub].append(
                    send(piece, piece, st.at[mask, sub, number], rt.at[mask, sub, number], peer)
                )
                number += 1

    def conclude(mask):
        for sub in range(units):
            for copy in far[mask, sub]:
                copy.wait_recv()
        place = table.at[pl.ds(spot(mask, 0, 0), times * block)]
        return send(place, place, sd.at[mask], rd.at[mask], partner)

    for sub in range(units):
        pixels = run // units

        starts = [sub * pixels + start for start in range(0, pixels, SUB)]
        entry = [
            jnp.concatenate([mine[pl.ds(start * ROWS + row, SUB, stride=ROWS), :] for start in starts], axis=0)
            for row in range(ROWS)
        ]
        answer = damped_solve(entry[:15], entry[15:], 5, SOURCE_PAIRS)
        for c in range(UPD):
            for number, start in enumerate(starts):
                upd[pl.ds(start * UPD + c, SUB, stride=UPD), :] = answer[c][number * SUB : (number + 1) * SUB]
        for mask in even + [1]:
            from_line[mask, sub] = send(
                upd.at[pl.ds(sub * unit, unit)], table.at[pl.ds(spot(0, time, sub), unit)],
                su.at[mask, sub], ru.at[mask, sub], line_peer[mask],
            )
        spread(0, sub)
        table[pl.ds(spot(0, time, sub), unit), :] = upd[sub * unit : (sub + 1) * unit, :]

    ordered = [0, 1] + even[::-1] + odd[::-1]
    def each(step, *group):
        for mask in group:
            for sub in range(units):
                step(mask, sub)

    each(spread, 1, *even[::-1])
    each(relay, 0, 1)
    each(spread, *odd[::-1])
    each(relay, *even[::-1])
    last = [conclude(0)]
    each(relay, *odd[::-1])
    last += [conclude(mask) for mask in ordered[1:]]
    for copy in last:
        copy.wait_recv()
    for copy in pending:
        copy.wait_send()


def exchange(sums, obs_weight, attitude_partials):
    times, owners = lax.axis_size("tm"), lax.axis_size("sky")
    lines = owners // 2
    outer, inner = split_times(times)
    total_rows = sums.shape[0]
    chunk = total_rows // (owners * times)
    pixels = total_rows // ROWS
    block = chunk // ROWS * UPD
    far_rows = chunk // 5
    rest = chunk - far_rows
    subs = 2 if rest % 32 == 0 else 1
    units = 2 if block % 32 == 0 else 1
    rows = rest // subs
    quarter = max(rows, far_rows) // 2
    tiles = obs_weight.shape[0]
    count = lines * subs
    total = count + 1
    dma = pltpu.SemaphoreType.DMA
    vmem = pltpu.VMEM
    near = inner + outer - 2
    far = 2 * (inner - 1) * (outer - 1)
    f32 = jnp.float32

    def pair(*shape):
        return [dma(shape), dma(shape)]

    return pl.pallas_call(
        functools.partial(exchange_kernel, times, lines, subs, units, 2, far_rows),
        name="exchange",
        out_shape=(
            jax.ShapeDtypeStruct((pixels * UPD + SUB, LANES), f32),
            jax.ShapeDtypeStruct((tiles, LANES), f32),
        ),
        in_specs=[pl.BlockSpec(memory_space=pltpu.VMEM)] * 3,
        out_specs=(pl.BlockSpec(memory_space=pltpu.VMEM),) * 2,
        scratch_shapes=[
            vmem((count, times, rows, LANES), f32),
            vmem((lines, times, far_rows, LANES), f32),
            vmem((lines, times, far_rows, LANES), f32),
            vmem((total, max(inner - 1, 1), outer, quarter, LANES), f32),
            vmem((total, max(outer - 1, 1), inner, quarter, LANES), f32),
            vmem((total, max(outer - 1, 1), quarter, LANES), f32),
            vmem((total, max(inner - 1, 1), quarter, LANES), f32),
            vmem((count, rows, LANES), f32),
            vmem((count, rows, LANES), f32),
            vmem((chunk, LANES), f32),
            vmem((block, LANES), f32),
        ]
        + pair(count)
        + pair(lines)
        + pair(lines)
        + pair(total, max(inner - 1, 1), outer)
        + pair(total, max(outer - 1, 1), inner)
        + pair(total, max(outer - 1, 1))
        + pair(total, max(inner - 1, 1))
        + pair(count)
        + pair(lines, units)
        + pair(lines, units, near + far)
        + pair(lines),
        compiler_params=pltpu.CompilerParams(
            collective_id=0, has_side_effects=True, vmem_limit_bytes=24 * MIB
        ),
    )(sums.reshape(lines, 2, times, chunk, LANES), obs_weight, attitude_partials)


def thirds(value):
    high = value.astype(jnp.bfloat16)
    rest = value - high.astype(jnp.float32)
    middle = rest.astype(jnp.bfloat16)
    return high, middle, (rest - middle.astype(jnp.float32)).astype(jnp.bfloat16)


def settle_kernel(
    times, owners, span, pixel_hbm, slot_hbm, knots, resid, weight, parts, att, index, table, squares,
    out, source_out, knot_out, pixel_ref, slot_ref, rows, terms, sums, before, mine, after, settles, values, others, gathered,
    sp, sl, sa, ra, sb, rb, sc, rc, sd, rd,
):
    mesh_ids = pl.DeviceIdType.MESH
    time, sky = lax.axis_index("tm"), lax.axis_index("sky")
    blocks = times * owners
    block = time * owners + sky
    nxt, prev = lax.rem(block + 1, blocks), lax.rem(block + blocks - 1, blocks)
    next_id, prev_id = (nxt // owners, lax.rem(nxt, owners)), (prev // owners, lax.rem(prev, owners))
    peers = [(time, lax.rem(sky + step, owners)) for step in range(1, owners)]
    barrier = pltpu.get_barrier_semaphore()
    edge_id = (lax.rem(time + times - 1, times), owners - 1)
    for peer in [next_id, prev_id, edge_id] + peers:
        pl.semaphore_signal(barrier, inc=1, device_id=peer, device_id_type=mesh_ids)

    pixels_in = pltpu.make_async_copy(pixel_hbm, pixel_ref, sp)
    slots_in = pltpu.make_async_copy(slot_hbm, slot_ref, sl)
    pixels_in.start()
    slots_in.start()
    pixels_in.wait()
    slots_in.wait()
    tiles = resid.shape[0]
    lane = lax.broadcasted_iota(jnp.int32, (SUB, LANES), 1)
    unroll = rows.shape[0]

    def group(step, carry):
        for part in range(unroll):
            base = pl.multiple_of((step * unroll + part) * SUB, SUB)
            here = pl.ds(base, SUB)
            for j in range(SUB):
                seat = slot_ref[pixel_ref[base + j]]
                rows[part, j * SUB : (j + 1) * SUB, :] = table[pl.ds(seat * UPD, SUB), :]
            ids = index[here, :]
            total = None
            for c in range(UPD):
                picked = jnp.take_along_axis(rows[part, pl.ds(c, SUB, stride=SUB), :], ids, axis=1)
                addend = parts[c, here, :] * picked
                total = addend if total is None else total + addend
            settled = resid[here, :] - total
            settles[here, :] = settled
            scaled = weight[here, :] * settled
            term = squares[here, :]
            for m in range(4):
                for c in range(4):
                    value = jnp.sum(scaled * att[4 * m + c, here, :], axis=1, keepdims=True)
                    term = jnp.where(lane == 16 * m + 10 + c, value, term)
            terms[here, :] = term
        return carry

    lax.fori_loop(0, tiles // (SUB * unroll), group, 0)
    knot = lax.broadcasted_iota(jnp.int32, (LANES, tiles), 0) + block * span
    hits = jnp.where(knot == knots[...], 1.0, 0.0).astype(jnp.bfloat16)
    placed = None
    for piece in thirds(terms[...]):
        got = jnp.dot(hits, piece, preferred_element_type=jnp.float32)
        placed = got if placed is None else placed + got
    turned = placed.T
    total = turned[:16]
    for m in range(1, 4):
        total = total + pltpu.roll(turned[16 * m : 16 * m + 16], m, 1)
    sums[...] = total

    last_of = sky == owners - 1
    pl.semaphore_wait(barrier, owners + 1 + jnp.where(last_of, owners, 0))
    pending = []

    def send(source, target, send_sem, recv_sem, peer):
        copy = pltpu.make_async_remote_copy(
            src_ref=source, dst_ref=target, send_sem=send_sem, recv_sem=recv_sem,
            device_id=peer, device_id_type=mesh_ids,
        )
        copy.start()
        pending.append(copy)
        return copy

    handed = [send(sums, before, sa, ra, next_id), send(sums, after, sb, rb, prev_id)]
    around = [
        send(sums, gathered.at[pl.ds((sky + 1) * 16, 16)], sc.at[number], rc.at[number], peer)
        for number, peer in enumerate(peers)
    ]
    edges = [
        pltpu.make_async_remote_copy(
            src_ref=sums, dst_ref=gathered.at[pl.ds(0, 16)], send_sem=sd.at[number], recv_sem=rd,
            device_id=(lax.rem(time + 1, times), number), device_id_type=mesh_ids,
        )
        for number in range(owners)
    ]

    @pl.when(last_of)
    def _():
        for copy in edges:
            copy.start()

    gathered[pl.ds(pl.multiple_of((sky + 1) * 16, 16), 16), :] = sums[...]
    per_owner = source_out.shape[1] // LANES

    def spread(step, carry):
        for part in range(SUB):
            pixel = step * SUB + part
            place = pl.ds(pl.multiple_of(pixel * LANES, LANES), LANES)
            source_out[:, place] = table[pl.ds((sky * per_owner + pixel) * UPD, UPD), :]
        return carry

    lax.fori_loop(0, per_owner // SUB, spread, 0)
    wide = lax.broadcasted_iota(jnp.int32, (16, LANES), 1)
    for copy in handed:
        copy.wait_recv()
    head = pltpu.roll(before[...], LANES - span, 1)
    tail = pltpu.roll(after[...], span, 1)
    whole = sums[...] + jnp.where((wide < 3) & (block > 0), head, 0.0)
    whole = whole + jnp.where((wide >= span) & (wide < span + 3), tail, 0.0)
    answer = damped_solve(
        [whole[n : n + 1] for n in range(10)], [whole[n : n + 1] for n in range(10, 14)], 4, KNOT_PAIRS
    )
    for c in range(4):
        mine[c : c + 1, :] = answer[c]
        mine[4 + c : 5 + c, :] = answer[c]
    reach = jnp.where(block < blocks - 1, span + 3, span)
    extended = jnp.where(lane < reach, mine[...], 0.0)
    windows = []
    for m in range(0, 4, 2):
        low = extended if m == 0 else pltpu.roll(extended, LANES - m, 1)
        high = pltpu.roll(extended, LANES - m - 1, 1)
        half = lax.broadcasted_iota(jnp.int32, (SUB, LANES), 0) < 4
        windows.append(jnp.where(half, low, high))
    window = jnp.concatenate(windows, axis=0)
    picked = None
    for piece in thirds(window):
        got = jnp.dot(piece, hits, preferred_element_type=jnp.float32)
        picked = got if picked is None else picked + got
    for part in range(tiles // LANES):
        values[part * LANES : (part + 1) * LANES, :] = picked[:, part * LANES : (part + 1) * LANES].T

    def last(step, carry):
        for part in range(unroll):
            here = pl.ds(pl.multiple_of((step * unroll + part) * SUB, SUB), SUB)
            column = values[here, :]
            total = None
            for number in range(16):
                addend = att[number, here, :] * column[:, number : number + 1]
                total = addend if total is None else total + addend
            out[here, :] = settles[here, :] - total
        return carry

    lax.fori_loop(0, tiles // (SUB * unroll), last, 0)
    for copy in around:
        copy.wait_recv()
    edges[0].wait_recv()
    lane_all = lax.broadcasted_iota(jnp.int32, (owners, LANES), 1)
    row_all = lax.broadcasted_iota(jnp.int32, (owners, LANES), 0)
    entering = (lane_all < 3) & ((row_all > 0) | (time > 0))
    wholes = []
    for row in range(14):
        head = pltpu.roll(gathered[pl.ds(row, owners, stride=16), :], LANES - span, 1)
        wholes.append(gathered[pl.ds(16 + row, owners, stride=16), :] + jnp.where(entering, head, 0.0))
    answer = damped_solve(wholes[:10], wholes[10:], 4, KNOT_PAIRS)
    for c in range(4):
        others[pl.ds(c, owners, stride=SUB), :] = answer[c]
    each = LANES // span
    for first in range(0, owners, each):
        joined = jnp.where(lane < span, others[first * SUB : (first + 1) * SUB, :], 0.0)
        for number in range(1, each):
            block_at = (first + number) * SUB
            moved = pltpu.roll(others[block_at : block_at + SUB, :], number * span, 1)
            keep = (lane >= number * span) & (lane < (number + 1) * span)
            joined = jnp.where(keep, moved, joined)
        knot_out[:, first * span : first * span + LANES] = joined[:4]
    for copy in pending:
        copy.wait_send()

    @pl.when(last_of)
    def _():
        for copy in edges:
            copy.wait_send()


def settle(tile_pixel, pixel_slot, knots, residual, obs_weight, source_partials, attitude_partials, source_index, table, squares, span):
    times, owners = lax.axis_size("tm"), lax.axis_size("sky")
    tiles = residual.shape[0]
    unroll = 8
    pixels = pixel_slot.shape[0]
    dma = pltpu.SemaphoreType.DMA
    f32 = jnp.float32
    return pl.pallas_call(
        functools.partial(settle_kernel, times, owners, span),
        name="settle",
        out_shape=(
            jax.ShapeDtypeStruct(residual.shape, f32),
            jax.ShapeDtypeStruct((UPD, pixels // owners * LANES), f32),
            jax.ShapeDtypeStruct((4, span * owners), f32),
        ),
        in_specs=[pl.BlockSpec(memory_space=pltpu.HBM)] * 2 + [pl.BlockSpec(memory_space=pltpu.VMEM)] * 8,
        out_specs=(pl.BlockSpec(memory_space=pltpu.VMEM),) * 3,
        scratch_shapes=[
            pltpu.SMEM(tile_pixel.shape, jnp.int32),
            pltpu.SMEM(pixel_slot.shape, jnp.int32),
            pltpu.VMEM((unroll, SUB * SUB, LANES), f32),
            pltpu.VMEM((tiles, LANES), f32),
            pltpu.VMEM((16, LANES), f32),
            pltpu.VMEM((16, LANES), f32),
            pltpu.VMEM((SUB, LANES), f32),
            pltpu.VMEM((16, LANES), f32),
            pltpu.VMEM(residual.shape, f32),
            pltpu.VMEM((tiles, 16), f32),
            pltpu.VMEM((owners * SUB, LANES), f32),
            pltpu.VMEM(((owners + 1) * 16, LANES), f32),
            dma, dma, dma, dma, dma, dma, dma((owners - 1,)), dma((owners - 1,)), dma((owners,)), dma,
        ],
        compiler_params=pltpu.CompilerParams(
            collective_id=1, has_side_effects=True, vmem_limit_bytes=24 * MIB
        ),
    )(tile_pixel, pixel_slot, knots, residual, obs_weight, source_partials, attitude_partials, source_index, table, squares)


def finish_kernel(*refs):
    count = (len(refs) - 1) // 2
    copies = [
        pltpu.make_async_copy(refs[number], refs[count + number], refs[-1].at[number]) for number in range(count)
    ]
    for copy in copies:
        copy.start()
    for copy in copies:
        copy.wait()


def finish(*results):
    return pl.pallas_call(
        finish_kernel,
        name="finish",
        out_shape=tuple(jax.ShapeDtypeStruct(value.shape, value.dtype) for value in results),
        in_specs=[pl.BlockSpec(memory_space=pltpu.VMEM)] * len(results),
        out_specs=(pl.BlockSpec(memory_space=pltpu.HBM),) * len(results),
        scratch_shapes=[pltpu.SemaphoreType.DMA((len(results),))],
        compiler_params=pltpu.CompilerParams(vmem_limit_bytes=8 * MIB),
    )(*results)


def body(residual, obs_weight, source_partials, attitude_partials, source_index, tile_pixel, tile_knot, pixel_slot):
    span = KNOTS_DEV // lax.axis_size("sky")
    sums = local_sums(tile_pixel, pixel_slot, residual, obs_weight, source_partials, source_index)
    table, squares = exchange(sums, obs_weight, attitude_partials)
    results = settle(
        tile_pixel, pixel_slot, tile_knot[None, :], residual, obs_weight, source_partials,
        attitude_partials, source_index, table, squares, span,
    )
    return finish(*results)


def solution(mesh):
    in_specs = (
        P(("tm", "sky"), None),
        P(("tm", "sky"), None),
        P(None, ("tm", "sky"), None),
        P(None, ("tm", "sky"), None),
        P(("tm", "sky"), None),
        P(("tm", "sky")),
        P(("tm", "sky")),
        P(),
    )
    out_specs = (P(("tm", "sky"), None), P(None, "sky"), P(None, "tm"))
    return jax.shard_map(body, mesh=mesh, in_specs=in_specs, out_specs=out_specs, check_vma=False)
```
